32 devices in a mesh: bl: 8 (over y, x, core), bp: 4 (over z).
Axes of the slice: x: 2, y: 2, z: 4, core: 2. Of those that a mesh axis runs over, the one named last changes fastest.
Arguments:
- inverse_cov: float32 [8, 1024, 1024], P('bl', 'bp'), may hold values from -1 to 12, as said below
- channel_keep_mask: int32 [8, 1024], P('bl'), may hold values 0 or 1
- partner_ids: int32 [8, 2], P('bl'), may hold values from -1 to 7, as said below
- band_starts: int32 [2, 64], replicated, may hold values from 0 to 384
Outputs:
- fisher: float32 [2, 64, 64], P(None, 'bp', 'bl')
The draws below stay inside these ranges and needn't reach their ends.
Inputs may be any that keep to these rules, and one draw needn't show every extreme that they name: partner_ids[i, k] is -1 for an empty slot, else the index of a baseline whose group, its index // 1, lies 1 to 4 groups after the group of baseline i, counted cyclically over the 8 groups; in every draw some baseline has all 2 slots filled. Each inverse_cov[i] is symmetric.
All inputs are finite; a program needn't handle non-finite values. No bound on the sum of `channel_keep_mask` on one device may be relied on, other than what follows from the above.
Results may differ from the reference program's by a relative error of at most 0.0003.
Values sent between devices are 32-bit elements; how exact they have to be, the bound alone decides.
No kernel may reach another device: no remote copies, remote signals or barrier semaphores. Data moves between devices by JAX's collectives and lax.ppermute only.
A program may use at most 128 MiB of HBM per device.

```python
from functools import partial
import jax
import jax.numpy as jnp
from jax import lax

CHANNEL_COUNT = 1024
PANEL = 512
BANDPOWER_COUNT = 64
WINDOW_LENGTH = 128
PAIRS_PER_SHARD = 1
ANTENNA_PAIRS = 8
COMPANION_SEATS = 2
GROUP_REACH = 4


def draw_inverse_cov(key, part):
    seed_sequence = jax.random.split(key, 5)
    rough_estimate = jax.random.uniform(seed_sequence[0], (ANTENNA_PAIRS, CHANNEL_COUNT, CHANNEL_COUNT), jnp.float32, -1.0, 1.0)
    coupled = (rough_estimate + jnp.swapaxes(rough_estimate, 1, 2)) * (0.5 / 32.0)
    identity = jnp.eye(CHANNEL_COUNT, dtype=jnp.float32)
    diagonal_entries = jax.random.uniform(seed_sequence[1], (ANTENNA_PAIRS, CHANNEL_COUNT), jnp.float32, 1.0, 2.0)
    channel_weighting = jax.random.uniform(seed_sequence[2], (ANTENNA_PAIRS, CHANNEL_COUNT), jnp.float32, 0.5, 1.5)
    correlation_length = jnp.exp(jax.random.uniform(seed_sequence[3], (ANTENNA_PAIRS,), jnp.float32, jnp.log(CHANNEL_COUNT / 4.0), jnp.log(CHANNEL_COUNT * 1.0)))
    signal_amplitude = jax.random.uniform(seed_sequence[4], (ANTENNA_PAIRS,), jnp.float32, 0.04, 0.1)
    channel_pos = jnp.arange(CHANNEL_COUNT, dtype=jnp.float32)
    spread = jnp.abs(channel_pos[:, None] - channel_pos[None, :])
    smooth = signal_amplitude[:, None, None] * channel_weighting[:, :, None] * channel_weighting[:, None, :] * jnp.exp(-spread[None, :, :] / correlation_length[:, None, None])
    alternating = 1.0 - 2.0 * (jnp.arange(CHANNEL_COUNT, dtype=jnp.int32) % 2).astype(jnp.float32)
    parity = 0.1 * alternating[:, None] * alternating[None, :]
    matrix = coupled * (1.0 - identity) + identity * diagonal_entries[:, :, None] + smooth + parity[None, :, :]
    return matrix


def draw_partner_ids(key, part):
    seed_sequence = jax.random.split(key, 6)
    antenna_pair_sets = ANTENNA_PAIRS // PAIRS_PER_SHARD
    antenna_pair_number = jnp.arange(ANTENNA_PAIRS, dtype=jnp.int32)
    rotation_team = antenna_pair_number // PAIRS_PER_SHARD
    turn_shift = jax.random.randint(seed_sequence[0], (), 0, GROUP_REACH, dtype=jnp.int32)
    phase_bit = jax.random.randint(seed_sequence[1], (), 0, 2, dtype=jnp.int32)
    heaviest_group = jax.random.randint(seed_sequence[2], (), 0, ANTENNA_PAIRS, dtype=jnp.int32)
    additional_step = jax.random.randint(seed_sequence[3], (ANTENNA_PAIRS, COMPANION_SEATS), 0, GROUP_REACH, dtype=jnp.int32)
    team_element = jax.random.randint(seed_sequence[4], (ANTENNA_PAIRS, COMPANION_SEATS), 0, PAIRS_PER_SHARD, dtype=jnp.int32)
    keep_probability = jax.random.randint(seed_sequence[5], (ANTENNA_PAIRS, COMPANION_SEATS), 0, 10, dtype=jnp.int32)
    slot_ids = jnp.arange(COMPANION_SEATS, dtype=jnp.int32)[None, :]
    first_hop = ((rotation_team + turn_shift) % GROUP_REACH)[:, None]
    number_of_hops = 1 + jnp.where(slot_ids == 0, first_hop, additional_step)
    steady = ((rotation_team + phase_bit * GROUP_REACH) // GROUP_REACH % 2 == 0)[:, None] & (slot_ids == 0)
    filled = steady | (keep_probability < 3) | (antenna_pair_number == heaviest_group)[:, None]
    companion_pair = (rotation_team[:, None] + number_of_hops) % antenna_pair_sets * PAIRS_PER_SHARD + team_element
    return jnp.where(filled, companion_pair, -1).astype(jnp.int32)


def touch_ends(result, stream_key, low, top_value):
    shape = result.shape
    spot = [jax.random.randint(jax.random.fold_in(stream_key, axis), (), 0, shape[axis]) for axis in range(len(shape))]
    result = result.at[tuple(spot)].set(low)
    longest = shape.index(max(shape))
    spot[longest] = (spot[longest] + 1) % shape[longest]
    return result.at[tuple(spot)].set(top_value)


def setup_inputs(seed: int = 0) -> dict:
    keys = jax.random.split(jax.random.key(seed), 5)
    inverse_cov = draw_inverse_cov(jax.random.fold_in(keys[4], 71), 0)
    channel_keep_mask = touch_ends((jax.random.randint(keys[1], (ANTENNA_PAIRS, CHANNEL_COUNT), 0, 5) < 4).astype(jnp.int32), jax.random.fold_in(keys[1], 1), 0, 1)
    partner_ids = draw_partner_ids(jax.random.fold_in(keys[4], 71), 0)
    band_starts = touch_ends(jax.random.randint(keys[3], (2, BANDPOWER_COUNT), 0, PANEL - WINDOW_LENGTH + 1), jax.random.fold_in(keys[3], 1), 0, PANEL - WINDOW_LENGTH).astype(jnp.int32)
    return dict(inverse_cov=inverse_cov, channel_keep_mask=channel_keep_mask, partner_ids=partner_ids, band_starts=band_starts)


highest = lax.Precision.HIGHEST


def kernel_stack(first_band, band_count, window):
    channel_pos = jnp.arange(window, dtype=jnp.float32)
    spread = jnp.abs(channel_pos[:, None] - channel_pos[None, :])
    band_ids = first_band + jnp.arange(band_count, dtype=jnp.int32)
    length = 1.0 + (band_ids % 4).astype(jnp.float32)
    return jnp.exp(-spread[None, :, :] / length[:, None, None])


def project(panel_block, starts, kernels):
    window = kernels.shape[1]
    window_rows = jax.vmap(lambda row_start: lax.dynamic_slice_in_dim(panel_block, row_start, window, 0))(starts)
    return jnp.einsum("apq,aqc->apc", kernels, window_rows, precision=highest, preferred_element_type=jnp.float32)


def column_windows(projected, starts, window):
    def one_matrix(matrix):
        return jax.vmap(lambda column_start: lax.dynamic_slice_in_dim(matrix, column_start, window, 1))(starts)
    return jax.vmap(one_matrix)(projected)


def baseline_panels(inverse_cov, channel_keep_mask, index):
    matrix = lax.dynamic_index_in_dim(inverse_cov, index, 0, keepdims=False)
    flag_marks = lax.dynamic_index_in_dim(channel_keep_mask, index, 0, keepdims=False).astype(jnp.float32)
    halves = []
    for half_index in range(2):
        lower = half_index * PANEL
        block_part = matrix[lower:lower + PANEL, lower:lower + PANEL]
        marks_half = flag_marks[lower:lower + PANEL]
        halves.append(block_part * marks_half[:, None] * marks_half[None, :])
    return halves


def pair_fisher(own_rows, partner_rows, starts):
    def one_band(inputs):
        partner_row, band_begin = inputs
        partner_windows = column_windows(partner_row[None], starts, WINDOW_LENGTH)[0]
        own_windows = column_windows(own_rows, band_begin[None], WINDOW_LENGTH)[:, 0]
        return jnp.einsum("bpq,bqp->b", partner_windows, own_windows, precision=highest, preferred_element_type=jnp.float32)
    return lax.map(one_band, (partner_rows, starts))


def slot_fisher(inverse_cov, channel_keep_mask, band_starts, kernels, own_rows, target):
    partner_halves = baseline_panels(inverse_cov, channel_keep_mask, target)
    results = []
    for half_index in range(2):
        partner_rows = project(partner_halves[half_index], band_starts[half_index], kernels)
        results.append(pair_fisher(own_rows[half_index], partner_rows, band_starts[half_index]))
    return jnp.stack(results)


def reference(inverse_cov, channel_keep_mask, partner_ids, band_starts):
    kernels = kernel_stack(0, BANDPOWER_COUNT, WINDOW_LENGTH)

    def accumulate_fisher(index, running_totals):
        own_halves = baseline_panels(inverse_cov, channel_keep_mask, index)
        own_rows = [project(own_halves[half_index], band_starts[half_index], kernels) for half_index in range(2)]
        for slot_index in range(COMPANION_SEATS):
            target = partner_ids[index, slot_index]
            safe_target = jnp.maximum(target, 0).astype(jnp.int32)
            running_totals = running_totals + lax.cond(target >= 0, partial(slot_fisher, inverse_cov, channel_keep_mask, band_starts, kernels, own_rows, safe_target), partial(jnp.zeros, (2, BANDPOWER_COUNT, BANDPOWER_COUNT), jnp.float32))
        return running_totals

    running_totals = lax.fori_loop(0, ANTENNA_PAIRS, accumulate_fisher, jnp.zeros((2, BANDPOWER_COUNT, BANDPOWER_COUNT), jnp.float32))
    return running_totals * (1.0 / (4 * ANTENNA_PAIRS * WINDOW_LENGTH))
```

```python
from functools import partial

import jax
import jax.numpy as jnp
from jax import lax
from jax.experimental import pallas as pl
from jax.experimental.pallas import tpu as pltpu
from jax.sharding import PartitionSpec as P

WINDOW = 128
KINDS = 4
GROUP_REACH = 4

f32 = jnp.float32
bf16 = jnp.bfloat16
SMEM = pl.BlockSpec(memory_space=pltpu.SMEM)
VMEM = pl.BlockSpec(memory_space=pltpu.VMEM)


def params(mib):
    return pltpu.CompilerParams(vmem_limit_bytes=mib << 20)


def dot(a, b):
    return jnp.dot(a, b, preferred_element_type=f32)


def split(x):
    high = x.astype(bf16)
    return high, (x - high.astype(f32)).astype(bf16)


def left3(x):
    high, low = split(x)
    return jnp.concatenate([high, low, high], axis=1)


def right3(x):
    high, low = split(x)
    return jnp.concatenate([high, high, low], axis=0)


def dot3(a, b):
    return dot(left3(a), right3(b))


def iota(shape, dim):
    return lax.broadcasted_iota(jnp.int32, shape, dim)


def block_place(place, block):
    return jnp.where(place == 0, block, jnp.where(block < 2, block + 2, 3 - block))


def positions(place, count, dim, shape, block):
    index = iota(shape, dim)
    other = index + jnp.where(index < 2 * block, 2, jnp.where(index < 3 * block, -1, -3)) * block
    return jnp.where(place == 0, index, other).astype(f32)


def pack_kernel(sc, pid, cov, keep, panel_out, diag_out, pack_out):
    place, group = sc[1], sc[3]
    rows, width = cov.shape[1], cov.shape[2]
    block = rows // 2
    marks = keep[...].astype(f32)
    half_marks = jnp.where(sc[0] == 0, marks[:, :width], marks[:, width:])
    row_marks = jnp.where(place == 0, half_marks[:, :rows], half_marks[:, rows:])
    row_col = jnp.transpose(jnp.broadcast_to(row_marks, (128, rows)))[:, :1]
    masked = cov[0] * row_col * half_marks
    first = place == 0
    own = jnp.where(first, masked[:, :rows], masked[:, rows:])
    c0 = jnp.where(first, masked[:, 2 * block : 3 * block], masked[:, block : 2 * block])
    c1 = jnp.where(first, masked[:, 3 * block :], masked[:, :block])
    panel_out[:, :rows] = own
    panel_out[:, rows : rows + block] = c0
    panel_out[:, rows + block :] = c1
    d00, d01 = own[:block, :block], own[:block, block:]
    d10, d11 = own[block:, :block], own[block:, block:]
    diag_out[:block, :block] = jnp.where(first, d11, d00)
    diag_out[:block, block:] = jnp.where(first, d10, d01)
    diag_out[block:, :block] = jnp.where(first, d01, d10)
    diag_out[block:, block:] = jnp.where(first, d00, d11)
    above = iota((block, block), 0) < iota((block, block), 1)
    on = iota((block, block), 0) == iota((block, block), 1)
    pack_out[:block] = d01
    pack_out[block : 2 * block] = jnp.where(above, d00, d11)
    pack_out[2 * block : 3 * block] = c0[:block]
    pack_out[3 * block : 4 * block] = c1[block:]
    diag = jnp.sum(jnp.where(on, d00, 0.0), axis=0, keepdims=True)
    slots = pid.shape[1]
    line = iota((8, block), 0)
    extra = jnp.where(line == 0, diag, 0.0)
    extra = jnp.where(line == 1, group.astype(f32), extra)
    for slot in range(slots):
        extra = jnp.where(line == 2 + slot, pid[0, slot].astype(f32), extra)
    pack_out[4 * block :] = extra


def start_rows(sc, starts):
    row = jnp.where(sc[0] == 0, starts[0:1, :], starts[1:2, :]).astype(f32)
    row = jnp.concatenate([row, row], axis=1)
    column = jnp.transpose(jnp.broadcast_to(row, (row.shape[1], row.shape[1])))[:, :1]
    return row, column


def rate(shape, dim):
    return -1.0 / (1 + iota(shape, dim) % KINDS).astype(f32)


def outside(offset, decay, side):
    before = jnp.where(offset < 0, jnp.exp(jnp.minimum(-1.0 - offset, 1e4).clip(0.0) * decay), 0.0)
    past = offset - WINDOW
    after = jnp.where(past >= 0, jnp.exp(past.clip(0.0) * decay), 0.0)
    return jnp.where(side, after, before)


def inside(offset, decay, side):
    held = (offset >= 0) & (offset < WINDOW)
    length = jnp.where(side, WINDOW - offset, offset + 1.0)
    return jnp.where(held, jnp.exp(jnp.where(held, length, 0.0) * decay), 0.0)


def filter_kernel(
    sc, starts, panel, other,
    td_out, to_out, hd_out, h0_out, h1_out, g_out, q_out,
    p3, gd, g0, g1, gr, w3, k3,
):
    place = sc[1]
    rows, width = panel.shape
    block = rows // 2
    bands = 2 * starts.shape[1]
    for at, value in ((slice(0, rows), panel[...]),):
        high, low = split(value)
        p3[0:rows, :] = high
        p3[width : width + rows, :] = high
        p3[2 * width : 2 * width + rows, :] = low
    turned = jnp.transpose(panel[:, rows:])
    high, low = split(turned)
    p3[rows:width, :rows] = high
    p3[width + rows : 2 * width, :rows] = high
    p3[2 * width + rows :, :rows] = low
    high, low = split(other[...])
    p3[rows:width, rows:] = high
    p3[width + rows : 2 * width, rows:] = high
    p3[2 * width + rows :, rows:] = low

    lanes = positions(place, width, 1, (block, width), block)

    def spread_of(index):
        base = block_place(place, index) * block
        return jnp.abs((base + iota((block, width), 0)).astype(f32) - lanes)

    def fill(index, carry):
        spread = spread_of(index)
        at = pl.multiple_of(index * block, block)
        for kind in range(KINDS):
            high, low = split(jnp.exp(spread / -(1.0 + kind)))
            for third, part in enumerate((high, high, low)):
                here = pl.ds(third * width + at, block)
                gd[here, kind * rows : (kind + 1) * rows] = part[:, :rows]
                g0[here, kind * block : (kind + 1) * block] = part[:, rows : rows + block]
                g1[here, kind * block : (kind + 1) * block] = part[:, rows + block :]
        return carry

    lax.fori_loop(0, width // block, fill, 0)

    def fill_rows(index, carry):
        spread = spread_of(index)
        for kind in range(KINDS):
            high, low = split(jnp.exp(spread / -(1.0 + kind)))
            here = pl.ds(pl.multiple_of(kind * rows + index * block, block), block)
            for third, part in enumerate((high, low, high)):
                gr[here, third * width : (third + 1) * width] = part
        return carry

    lax.fori_loop(0, 2, fill_rows, 0)

    row, column = start_rows(sc, starts)
    shape = (width, bands)
    offset = positions(place, width, 0, shape, block) - row
    k3[...] = right3(outside(offset, rate(shape, 1), iota(shape, 1) >= bands // 2))
    shape = (bands, width)
    offset = positions(place, width, 1, shape, block) - column
    weights = outside(offset, rate(shape, 0), iota(shape, 0) >= bands // 2)
    edge3 = left3(dot(left3(weights), p3[...]))
    for kind in range(KINDS):
        at = slice(kind * rows, (kind + 1) * rows)
        hd_out[:, at] = dot(edge3, gd[:, at])
    h0_out[...] = dot(edge3, g0[...])
    h1_out[...] = dot(edge3, g1[...])
    q_out[...] = dot(edge3, k3[...])

    def work(kind, carry):
        at = pl.ds(pl.multiple_of(kind * rows, rows), rows)
        value = dot(gr[at, :], p3[...])
        high, low = split(value)
        w3[:, :width] = high
        w3[:, width : 2 * width] = low
        w3[:, 2 * width :] = high
        for second in range(KINDS):
            here = slice(second * rows, (second + 1) * rows)
            td_out[at, here] = dot(w3[...], gd[:, here])
        for second in range(0, KINDS, 2):
            here = slice(second * block, (second + 2) * block)
            top = pl.ds(pl.multiple_of(kind * rows, block), block)
            low_rows = pl.ds(pl.multiple_of(kind * rows + block, block), block)
            to_out[top, here] = dot(w3[:block, :], g0[:, here])
            to_out[low_rows, here] = dot(w3[block:, :], g1[:, here])
        g_out[at, :] = dot(w3[...], k3[...])
        return carry

    lax.fori_loop(0, KINDS, work, 0)


def dot2(a, b):
    high, low = split(b)
    return dot(a, high) + dot(a, low)


def contract_kernel(
    peer_counts, scale, sc, pid, starts, *refs
):
    count = len(peer_counts)
    packs = refs[:count]
    td, to, hd, h0, h1, g, q, out, m_box, edges, final = refs[count:]
    place, group = sc[1], sc[3]
    rows = td.shape[0] // KINDS
    block = rows // 2
    slots = pid.shape[1]
    half_bands = starts.shape[1]
    bands = 2 * half_bands
    total = extra = None
    for pack, both in zip(packs, peer_counts):
        aux = pack[4 * block :, :]
        source = aux[1:2, :]
        weight = jnp.zeros_like(source)
        for slot in range(slots):
            weight = weight + jnp.where(source == pid[0, slot].astype(f32), 1.0, 0.0)
            if both:
                weight = weight + jnp.where(
                    aux[2 + slot : 3 + slot, :] == group.astype(f32), 1.0, 0.0
                )
        part = pack[: 4 * block, :] * weight
        line = aux[0:1, :] * weight
        total = part if total is None else total + part
        extra = line if extra is None else extra + line
    tri = total[block : 2 * block]
    above = iota((block, block), 0) < iota((block, block), 1)
    on = iota((block, block), 0) == iota((block, block), 1)
    s00 = jnp.where(above, tri, jnp.where(on, 0.5 * extra, 0.0))
    s11 = jnp.where(above, 0.0, jnp.where(on, 0.5 * tri, tri))
    zero = jnp.zeros((block, block), f32)
    s_top = jnp.concatenate([s00, total[:block]], axis=1)
    s_low = jnp.concatenate([zero, s11], axis=1)
    s_own = jnp.concatenate([s_top, s_low], axis=0)
    s_c0 = total[2 * block : 3 * block]
    s_c1 = total[3 * block :]

    row, column = start_rows(sc, starts)
    b_row = row[:, :half_bands]

    def boxes(count, base):
        shape = (KINDS * count, half_bands)
        index = iota(shape, 0)
        kind = index // count
        offset = (base + index % count).astype(f32) - b_row
        hit = (offset >= 0) & (offset < WINDOW) & (iota(shape, 1) % KINDS == kind)
        return jnp.where(hit, 1.0, 0.0).astype(bf16)

    own_base = place * rows
    box_own = boxes(rows, own_base)
    box_c0 = boxes(block, block_place(place, 2) * block)
    box_c1 = boxes(block, block_place(place, 3) * block)

    shape = (bands, rows)
    offset = (own_base + iota(shape, 1)).astype(f32) - column
    reach_rows = inside(offset, rate(shape, 0), iota(shape, 0) >= half_bands)
    shape = (2 * rows, bands)
    offset = positions(place, 2 * rows, 0, shape, block) - row
    reach_cols = inside(offset, rate(shape, 1), iota(shape, 1) >= half_bands)

    v_top = dot3(
        jnp.concatenate([s_top, s_c0], axis=1), reach_cols[: 3 * block]
    )
    v_low = dot3(
        jnp.concatenate([s_low, s_c1], axis=1),
        jnp.concatenate([reach_cols[:rows], reach_cols[3 * block :]], axis=0),
    )
    v = jnp.concatenate([v_top, v_low], axis=0)
    y_own = dot3(reach_rows, s_own)
    y_c0 = dot3(reach_rows[:, :block], s_c0)
    y_c1 = dot3(reach_rows[:, block:], s_c1)

    pair0 = jnp.concatenate([s_c0, s_c0], axis=1)
    pair1 = jnp.concatenate([s_c1, s_c1], axis=1)

    def boxed(x, box):
        high, low = split(x)
        return dot(high, box) + dot(low, box)

    for kind in range(KINDS):
        top, low_rows = kind * rows, kind * rows + block
        at = slice(top, top + rows)
        acc = jnp.zeros((rows, half_bands), f32)
        acc_top = jnp.zeros((block, half_bands), f32)
        acc_low = jnp.zeros((block, half_bands), f32)
        for second in range(KINDS):
            here = slice(second * rows, (second + 1) * rows)
            acc = acc + boxed(s_own * td[at, here], box_own[here])
        for second in range(0, KINDS, 2):
            here = slice(second * block, (second + 2) * block)
            acc_top = acc_top + boxed(pair0 * to[top:low_rows, here], box_c0[here])
            acc_low = acc_low + boxed(pair1 * to[low_rows : top + rows, here], box_c1[here])
        m_box[top:low_rows, :] = acc[:block] + acc_top
        m_box[low_rows : top + rows, :] = acc[block:] + acc_low
        edges[at, :] = v * g[at, :]

    shape = (half_bands, KINDS * rows)
    index = iota(shape, 1)
    offset = (own_base + index % rows).astype(f32) - column[:half_bands]
    hit = (offset >= 0) & (offset < WINDOW) & (iota(shape, 0) % KINDS == index // rows)
    box_rows = jnp.where(hit, 1.0, 0.0).astype(bf16)
    plain = dot2(box_rows, m_box[...])
    third = dot2(box_rows, edges[...])
    second = jnp.zeros((bands, half_bands), f32)
    for kind in range(KINDS):
        here = slice(kind * rows, (kind + 1) * rows)
        second = second + boxed(y_own * hd[:, here], box_own[here])
        here = slice(kind * block, (kind + 1) * block)
        second = second + boxed(y_c0 * h0[:, here], box_c0[here])
        second = second + boxed(y_c1 * h1[:, here], box_c1[here])
    fourth = dot3(reach_rows, v) * q[...]
    third = third - fourth[:half_bands] - fourth[half_bands:]
    result = plain - second[:half_bands] - second[half_bands:]
    result = result - third[:, :half_bands] - third[:, half_bands:]
    final[...] = jnp.zeros(final.shape, f32)
    final[:half_bands, :half_bands] = result
    whole = final[...]
    final[...] = (whole + jnp.transpose(whole)) * scale
    share = out.shape[1]
    owners = out.shape[0] * share // half_bands
    for index in range(out.shape[0]):
        first = index // owners * share
        out[index] = final[first : first + share, :half_bands]


def gather_kernel(owners, sc, parts, out, buffer):
    share, bands = parts.shape[1], parts.shape[2]
    per_half = owners // 2
    buffer[...] = jnp.zeros(buffer.shape, f32)
    for half in range(2):
        acc = None
        for first in range(0, parts.shape[0], owners):
            for place in range(per_half):
                value = parts[first + half * per_half + place]
                acc = value if acc is None else acc + value
        buffer[:share, :bands] = acc
        buffer[...] = jnp.transpose(buffer[...])
        lines = out.shape[1]
        start = pl.multiple_of(sc[2] * lines, 8)
        out[half] = buffer[pl.ds(start, lines), :share]


def partner_routes(groups):
    if groups == 2 * GROUP_REACH:
        routes = []
        for step in (3, 1, 2):

            def target(source, step=step):
                team, member = divmod(source, 2)
                goal = team ^ step
                return goal * 2 + (member if team < goal else 1 - member)

            routes.append(([(source, target(source)) for source in range(groups)], True))
        routes.append(([(source, source ^ 1) for source in range(groups)], False))
        return routes
    return [
        ([(source, (source - hop) % groups) for source in range(groups)], False)
        for hop in range(1, GROUP_REACH + 1)
    ]


def body(inverse_cov, channel_keep_mask, partner_ids, band_starts):
    local_count, rows, channels = inverse_cov.shape
    width = channels // 2
    block = rows // 2
    bands = band_starts.shape[1]
    groups, owners = lax.axis_size("bl"), lax.axis_size("bp")
    per_half = owners // 2
    assert local_count == 1 and width == 2 * rows and block == 128 == 2 * bands
    owner, group = lax.axis_index("bp"), lax.axis_index("bl")
    sc = jnp.stack([owner // per_half, owner % per_half, owner, group]).astype(jnp.int32)
    panel, diag, pack = pl.pallas_call(
        pack_kernel,
        grid_spec=pltpu.PrefetchScalarGridSpec(
            num_scalar_prefetch=2,
            grid=(1,),
            in_specs=[
                pl.BlockSpec((1, rows, width), lambda i, sc, pid: (0, 0, sc[0])),
                pl.BlockSpec((1, channels), lambda i, sc, pid: (0, 0)),
            ],
            out_specs=[
                pl.BlockSpec((rows, width), lambda i, sc, pid: (0, 0)),
                pl.BlockSpec((rows, rows), lambda i, sc, pid: (0, 0)),
                pl.BlockSpec((4 * block + 8, block), lambda i, sc, pid: (0, 0)),
            ],
        ),
        out_shape=[
            jax.ShapeDtypeStruct((rows, width), f32),
            jax.ShapeDtypeStruct((rows, rows), f32),
            jax.ShapeDtypeStruct((4 * block + 8, block), f32),
        ],
        compiler_params=params(16),
    )(sc, partner_ids, inverse_cov, channel_keep_mask)

    other = lax.ppermute(diag, "bp", [(place, place ^ 1) for place in range(owners)])
    routes = partner_routes(groups)
    packs = [lax.ppermute(pack, "bl", route) for route, _ in routes]

    shapes = [
        (KINDS * rows, KINDS * rows),
        (KINDS * rows, KINDS * block),
        (2 * bands, KINDS * rows),
        (2 * bands, KINDS * block),
        (2 * bands, KINDS * block),
        (KINDS * rows, 2 * bands),
        (2 * bands, 2 * bands),
    ]
    tables = pl.pallas_call(
        filter_kernel,
        in_specs=[SMEM, VMEM, VMEM, VMEM],
        out_specs=[VMEM] * 7,
        out_shape=[jax.ShapeDtypeStruct(shape, f32) for shape in shapes],
        scratch_shapes=[
            pltpu.VMEM((3 * width, width), bf16),
            pltpu.VMEM((3 * width, KINDS * rows), bf16),
            pltpu.VMEM((3 * width, KINDS * block), bf16),
            pltpu.VMEM((3 * width, KINDS * block), bf16),
            pltpu.VMEM((KINDS * rows, 3 * width), bf16),
            pltpu.VMEM((rows, 3 * width), bf16),
            pltpu.VMEM((3 * width, 2 * bands), bf16),
        ],
        compiler_params=params(40),
        cost_estimate=pl.CostEstimate(
            flops=9_000_000_000, bytes_accessed=8 << 20, transcendentals=1 << 21
        ),
    )(sc, band_starts, panel, other)

    scale = 1.0 / (4 * local_count * groups * WINDOW)
    share = bands // groups
    parts = pl.pallas_call(
        partial(contract_kernel, [both for _, both in routes], scale),
        in_specs=[SMEM, SMEM, VMEM] + [VMEM] * (len(routes) + 7),
        out_specs=VMEM,
        out_shape=jax.ShapeDtypeStruct((groups * owners, share, bands), f32),
        scratch_shapes=[
            pltpu.VMEM((KINDS * rows, bands), f32),
            pltpu.VMEM((KINDS * rows, 2 * bands), f32),
            pltpu.VMEM((128, 128), f32),
        ],
        compiler_params=params(30),
    )(sc, partner_ids, band_starts, *packs, *tables)

    met = lax.all_to_all(parts, ("bl", "bp"), 0, 0, tiled=True)
    return pl.pallas_call(
        partial(gather_kernel, owners),
        in_specs=[SMEM, VMEM],
        out_specs=VMEM,
        out_shape=jax.ShapeDtypeStruct((2, bands // owners, share), f32),
        scratch_shapes=[pltpu.VMEM((128, 128), f32)],
        compiler_params=params(8),
    )(sc, met)


def solution(mesh):
    placed = (P("bl", "bp", None), P("bl", None), P("bl", None), P())
    return jax.shard_map(
        body, mesh=mesh, in_specs=placed, out_specs=P(None, "bp", "bl"), check_vma=False
    )
```

```python
from functools import partial

import jax
import jax.numpy as jnp
from jax import lax
from jax.experimental import pallas as pl
from jax.experimental.pallas import tpu as pltpu
from jax.sharding import PartitionSpec as P

WINDOW = 128
KINDS = 4
GROUP_REACH = 4

f32 = jnp.float32
bf16 = jnp.bfloat16
SMEM = pl.BlockSpec(memory_space=pltpu.SMEM)
VMEM = pl.BlockSpec(memory_space=pltpu.VMEM)
HBM = pl.BlockSpec(memory_space=pltpu.HBM)


def params(mib):
    return pltpu.CompilerParams(vmem_limit_bytes=mib << 20)


def dot(a, b):
    return jnp.dot(a, b, preferred_element_type=f32)


def split(x):
    high = x.astype(bf16)
    return high, (x - high.astype(f32)).astype(bf16)


def left3(x):
    high, low = split(x)
    return jnp.concatenate([high, low, high], axis=1)


def right3(x):
    high, low = split(x)
    return jnp.concatenate([high, high, low], axis=0)


def dot_t(a, b):
    return lax.dot_general(a, b, (((1,), (1,)), ((), ())), preferred_element_type=f32)


def iota(shape, dim):
    return lax.broadcasted_iota(jnp.int32, shape, dim)


def pack_kernel(
    sc, cov_hbm, keep_hbm, pid_hbm, starts_hbm, panel_out, diag_out, pack_out, info_out,
    cov, keep, pid, starts, sems,
):
    rows, width = cov.shape
    columns = pl.ds(pl.multiple_of(sc[0] * width, width), width)
    copies = [
        pltpu.make_async_copy(cov_hbm.at[0, :, columns], cov, sems.at[0]),
        pltpu.make_async_copy(keep_hbm, keep, sems.at[1]),
        pltpu.make_async_copy(pid_hbm, pid, sems.at[2]),
        pltpu.make_async_copy(starts_hbm, starts, sems.at[3]),
    ]
    for copy in copies:
        copy.start()
    for copy in copies:
        copy.wait()
    block = rows // 2
    first = sc[1] == 0
    marks = keep[...].astype(f32)
    half_marks = jnp.where(sc[0] == 0, marks[:, :width], marks[:, width:])
    row_marks = jnp.where(first, half_marks[:, :rows], half_marks[:, rows:])
    row_col = jnp.transpose(jnp.broadcast_to(row_marks, (128, rows)))[:, :1]
    masked = cov[...] * row_col * half_marks
    own = jnp.where(first, masked[:, :rows], masked[:, rows:])
    c0 = jnp.where(first, masked[:, 2 * block : 3 * block], masked[:, block : 2 * block])
    c1 = jnp.where(first, masked[:, 3 * block :], masked[:, :block])
    panel_out[:, :rows] = own
    panel_out[:, rows : rows + block] = c0
    panel_out[:, rows + block :] = c1
    d00, d01 = own[:block, :block], own[:block, block:]
    d10, d11 = own[block:, :block], own[block:, block:]
    diag_out[:block, :block] = jnp.where(first, d11, d00)
    diag_out[:block, block:] = jnp.where(first, d10, d01)
    diag_out[block:, :block] = jnp.where(first, d01, d10)
    diag_out[block:, block:] = jnp.where(first, d00, d11)
    above = iota((block, block), 0) < iota((block, block), 1)
    on = iota((block, block), 0) == iota((block, block), 1)
    pack_out[:block] = d01
    pack_out[block : 2 * block] = jnp.where(above, d00, d11)
    pack_out[2 * block : 3 * block] = c0[:block]
    pack_out[3 * block : 4 * block] = c1[block:]
    line = iota((8, block), 0)
    info = jnp.where(line == 0, jnp.sum(jnp.where(on, d00, 0.0), axis=0, keepdims=True), 0.0)
    info = jnp.where(line == 1, sc[3].astype(f32), info)
    for slot in range(pid.shape[1]):
        info = jnp.where(line == 2 + slot, pid[0, slot].astype(f32), info)
    begin = jnp.where(sc[0] == 0, starts[0:1, :], starts[1:2, :]).astype(f32)
    info = jnp.where(line == 7, jnp.concatenate([begin, begin], axis=1), info)
    pack_out[4 * block :] = info
    info_out[...] = info


def turn(x):
    return jnp.transpose(x)


def decay(shape, dim):
    return -1.0 / (1 + iota(shape, dim) % KINDS).astype(f32)


def held(offset):
    return (offset >= 0) & (offset < WINDOW)


def filter_kernel(
    sc, info, panel, other,
    td_out, to_out, hd_out, h0_out, h1_out, q_out,
    bd_out, b0_out, b1_out, br_out, rh_out, rl_out,
    p3, kr, kc0, kc1, kl,
):
    first = sc[1] == 0
    rows, width = panel.shape
    block = rows // 2
    twice = info.shape[1]
    bands = twice // 2

    high, low = split(panel[...])
    p3[0:rows, :] = high
    p3[rows : 2 * rows, :] = high
    p3[2 * rows : 3 * rows, :] = low
    high, low = split(turn(panel[:, rows:]))
    p3[3 * rows : 4 * rows, :rows] = high
    p3[4 * rows : 5 * rows, :rows] = high
    p3[5 * rows :, :rows] = low
    high, low = split(other[...])
    p3[3 * rows : 4 * rows, rows:] = high
    p3[4 * rows : 5 * rows, rows:] = high
    p3[5 * rows :, rows:] = low

    for chunk in range(2):
        shape = (block, rows)
        line = iota(shape, 0) + chunk * block
        lane = iota(shape, 1)
        spread = jnp.abs(line - lane).astype(f32)
        swapped = jnp.abs((line + block) % rows - (lane + block) % rows).astype(f32)
        cross = jnp.where(first, spread, swapped)
        here = chunk * block
        for kind in range(KINDS):
            at = slice(kind * rows, (kind + 1) * rows)
            high, low = split(jnp.exp(spread / -(1.0 + kind)))
            for third, part in enumerate((high, high, low)):
                kr[third * rows + here : third * rows + here + block, at] = part
            for third, part in enumerate((high, low, high)):
                kl[kind * rows + here : kind * rows + here + block,
                   third * rows : (third + 1) * rows] = part
            high, low = split(jnp.exp(cross / -(1.0 + kind)))
            at = slice(kind * block, (kind + 1) * block)
            for third, part in enumerate((high, high, low)):
                kc0[third * rows + here : third * rows + here + block, at] = part[:, :block]
                kc1[third * rows + here : third * rows + here + block, at] = part[:, block:]

    def own_place(index):
        return index + jnp.where(first, 0, rows)

    def other_place(index):
        return jnp.where(first, index + rows, (index + block) % rows)

    def gap(place):
        return jnp.abs(place.astype(f32) - (rows - 0.5))

    shape = (rows, twice)
    own_column = jnp.exp(gap(own_place(iota(shape, 0))) * decay(shape, 1))
    other_column = jnp.exp(gap(other_place(iota(shape, 0))) * decay(shape, 1))
    shape = (8, rows)
    own_row = jnp.exp(gap(own_place(iota(shape, 1))) * decay(shape, 0))
    other_row = jnp.exp(gap(other_place(iota(shape, 1))) * decay(shape, 0))

    begin = info[7:8, :]
    begin_column = turn(jnp.broadcast_to(begin, (twice, twice)))[:, :1]

    extra = 16
    shape = (twice, rows)
    after = iota(shape, 0) >= bands

    def outside(place):
        offset = place.astype(f32) - begin_column
        reach = jnp.where(after, offset - WINDOW, -1.0 - offset)
        return jnp.where(
            reach >= 0, jnp.exp(jnp.where(reach >= 0, reach, 0.0) * decay(shape, 0)), 0.0
        )

    def inside(place):
        offset = place.astype(f32) - begin_column
        reach = jnp.where(after, WINDOW - offset, offset + 1.0)
        return jnp.where(
            held(offset), jnp.exp(jnp.where(held(offset), reach, 0.0) * decay(shape, 0)), 0.0
        )

    none = jnp.zeros((8, rows), f32)
    four = iota((8, rows), 0) < KINDS
    out_own = outside(own_place(iota(shape, 1)))
    out_other = outside(other_place(iota(shape, 1)))
    weights_own = jnp.concatenate([out_own, jnp.where(four, 0.0, own_row), none], axis=0)
    weights_other = jnp.concatenate([out_other, jnp.where(four, other_row, 0.0), none], axis=0)
    lhs = jnp.concatenate([left3(weights_own), left3(weights_other)], axis=1)
    edge = dot(lhs, p3[...])
    edge_own = left3(edge[:, :rows])
    edge_other = left3(edge[:, rows:])
    from_other = dot(edge_other, right3(other_column))
    from_own = dot(edge_own, right3(own_column))
    near = jnp.concatenate([left3(edge[:twice, :rows]), left3(edge[:twice, rows:])], axis=1)
    flip_own, flip_own_low = split(out_own)
    flip_other, flip_other_low = split(out_other)
    q_out[...] = dot_t(
        near,
        jnp.concatenate(
            [flip_own, flip_own, flip_own_low, flip_other, flip_other, flip_other_low], axis=1
        ),
    )
    for kind in range(KINDS):
        at = slice(kind * rows, (kind + 1) * rows)
        full = dot(edge_own, kr[:, at]) + from_other[:, kind : kind + 1] * own_row[kind : kind + 1]
        hd_out[:, at] = full[:twice]
        turned = turn(full[twice : twice + 8])
        value = dot(kl[at, :], p3[: 3 * rows, :])
        value = value + own_column[:, kind : kind + 1] * edge[twice + kind : twice + kind + 1, :]
        left_own = left3(value[:, :rows])
        left_other = left3(value[:, rows:])
        for second in range(kind, KINDS):
            here = slice(second * rows, (second + 1) * rows)
            to = pair_index(kind, second) * rows
            td_out[to : to + rows, :] = (
                dot(left_own, kr[:, here])
                + turned[:, second : second + 1] * own_row[second : second + 1]
            )
        top = dot(left_other[:block], kc0[...])
        bottom = dot(left_other[block:], kc1[...])
        for second in range(KINDS):
            here = slice(second * block, (second + 1) * block)
            column = turned[:, KINDS + second : KINDS + second + 1]
            line = other_row[second : second + 1]
            to_out[kind * rows : kind * rows + block, here] = (
                top[:, here] + column[:block] * line[:, :block]
            )
            to_out[kind * rows + block : (kind + 1) * rows, here] = (
                bottom[:, here] + column[block:] * line[:, block:]
            )
    high0 = dot(edge_other[:twice], kc0[...])
    high1 = dot(edge_other[:twice], kc1[...])
    for kind in range(KINDS):
        here = slice(kind * block, (kind + 1) * block)
        column = from_own[:twice, kind : kind + 1]
        line = other_row[kind : kind + 1]
        h0_out[:, here] = high0[:, here] + column * line[:, :block]
        h1_out[:, here] = high1[:, here] + column * line[:, block:]

    begins = begin[:, :bands]

    def boxes(count, place):
        shape = (KINDS * count, bands)
        index = iota(shape, 0)
        hit = held(place(index % count).astype(f32) - begins)
        hit = hit & (iota(shape, 1) % KINDS == index // count)
        return jnp.where(hit, 1.0, 0.0).astype(bf16)

    bd_out[...] = boxes(rows, own_place)
    b0_out[...] = boxes(block, other_place)
    b1_out[...] = boxes(block, lambda index: other_place(index + block))
    shape2 = (bands, KINDS * rows)
    index = iota(shape2, 1)
    hit = held(own_place(index % rows).astype(f32) - begin_column[:bands])
    hit = hit & (iota(shape2, 0) % KINDS == index // rows)
    br_out[...] = jnp.where(hit, 1.0, 0.0).astype(bf16)
    high, low = split(inside(own_place(iota(shape, 1))))
    rh_out[:, :rows] = high
    rl_out[:, :rows] = low
    high, low = split(inside(other_place(iota(shape, 1))))
    rh_out[:, rows:] = high
    rl_out[:, rows:] = low


def pair_index(kind, second):
    return kind * KINDS - kind * (kind - 1) // 2 + second - kind


def contract_kernel(peer_counts, slots, scale, owners, info, *refs):
    count = len(peer_counts)
    packs = refs[:count]
    td, to, hd, h0, h1, q, bd, b0, b1, br, rh, rl, out, m_box, final = refs[count:]
    rows = td.shape[1]
    block = rows // 2
    bands = bd.shape[1]
    twice = 2 * bands
    own = info[...]
    total = extra = None
    for pack, both in zip(packs, peer_counts):
        aux = pack[4 * block :, :]
        weight = jnp.zeros_like(aux[:1])
        for slot in range(slots):
            at = slice(2 + slot, 3 + slot)
            weight = weight + jnp.where(aux[1:2] == own[at], 1.0, 0.0)
            if both:
                weight = weight + jnp.where(aux[at] == own[1:2], 1.0, 0.0)
        part = pack[: 4 * block, :] * weight
        line = aux[0:1, :] * weight
        total = part if total is None else total + part
        extra = line if extra is None else extra + line
    upper = total[:block]
    tri = total[block : 2 * block]
    flipped = turn(tri)
    above = iota((block, block), 0) < iota((block, block), 1)
    on = iota((block, block), 0) == iota((block, block), 1)
    s00 = jnp.where(above, tri, jnp.where(on, extra, flipped))
    s11 = jnp.where(above, flipped, tri)
    s_own = jnp.concatenate(
        [
            jnp.concatenate([s00, upper], axis=1),
            jnp.concatenate([turn(upper), s11], axis=1),
        ],
        axis=0,
    )
    s_c0 = total[2 * block : 3 * block]
    s_c1 = total[3 * block :]
    half_own = 0.5 * s_own
    pair0 = jnp.concatenate([s_c0, s_c0], axis=1)
    pair1 = jnp.concatenate([s_c1, s_c1], axis=1)

    def boxed(x, box):
        high, low = split(x)
        return dot(high, box) + dot(low, box)

    for kind in range(KINDS):
        top, mid, end = kind * rows, kind * rows + block, (kind + 1) * rows
        acc = jnp.zeros((rows, bands), f32)
        acc_top = jnp.zeros((block, bands), f32)
        acc_low = jnp.zeros((block, bands), f32)
        for second in range(kind, KINDS):
            here = slice(second * rows, (second + 1) * rows)
            at = pair_index(kind, second) * rows
            value = half_own if second == kind else s_own
            acc = acc + boxed(value * td[at : at + rows, :], bd[here, :])
        for second in range(0, KINDS, 2):
            here = slice(second * block, (second + 2) * block)
            acc_top = acc_top + boxed(pair0 * to[top:mid, here], b0[here, :])
            acc_low = acc_low + boxed(pair1 * to[mid:end, here], b1[here, :])
        m_box[top:mid, :] = acc[:block] + acc_top
        m_box[mid:end, :] = acc[block:] + acc_low
    high, low = split(m_box[...])
    result = dot(br[...], high) + dot(br[...], low)

    reach = (rh[:, :rows], rl[:, :rows])
    reach0 = (rh[:, :block], rl[:, :block])
    reach1 = (rh[:, block:rows], rl[:, block:rows])
    over0 = (rh[:, rows : rows + block], rl[:, rows : rows + block])
    over1 = (rh[:, rows + block :], rl[:, rows + block :])

    def three(a, b, multiply):
        return multiply(a[0], b[0]) + multiply(a[0], b[1]) + multiply(a[1], b[0])

    part_own, part0, part1 = split(s_own), split(s_c0), split(s_c1)
    y_own = three(reach, part_own, dot)
    y_off = jnp.concatenate([three(over0, part0, dot_t), three(over1, part1, dot_t)], axis=1)
    y_0 = three(reach0, part0, dot)
    y_1 = three(reach1, part1, dot)
    fourth = three(split(0.5 * y_own + y_off), reach, dot_t) * q[...]
    y_own = y_own + y_off
    second = jnp.zeros((twice, bands), f32)
    for kind in range(KINDS):
        here = slice(kind * rows, (kind + 1) * rows)
        second = second + boxed(y_own * hd[:, here], bd[here, :])
        here = slice(kind * block, (kind + 1) * block)
        second = second + boxed(y_0 * h0[:, here], b0[here, :])
        second = second + boxed(y_1 * h1[:, here], b1[here, :])
    fourth = fourth[:bands] + fourth[bands:]
    result = result - second[:bands] - second[bands:] + fourth[:, :bands] + fourth[:, bands:]
    final[...] = jnp.zeros(final.shape, f32)
    final[:bands, :bands] = result
    whole = final[...]
    final[...] = (whole + turn(whole)) * scale

    groups = out.shape[0] // owners
    share, lines = bands // groups, bands // owners
    lane = iota((groups, final.shape[1]), 1)
    for owner in range(owners):
        row = jnp.zeros((groups, final.shape[1]), f32)
        for member in range(share):
            value = final[pl.ds(member, groups, stride=share), :]
            move = (member - owner) * lines % final.shape[1]
            value = pltpu.roll(value, move, 1) if move else value
            row = jnp.where(lane // lines == member, value, row)
        for group in range(groups):
            out[group * owners + owner] = row[group : group + 1]


def gather_kernel(owners, parts, out):
    per_half = owners // 2
    lines, share = out.shape[1], out.shape[2]
    lanes = parts.shape[2]
    for half in range(2):
        acc = None
        for first in range(0, parts.shape[0], owners):
            for place in range(per_half):
                value = parts[first + half * per_half + place]
                acc = value if acc is None else acc + value
        line = iota((lanes, lanes), 0)
        table = jnp.zeros((lanes, lanes), f32)
        for member in range(share):
            value = pltpu.roll(acc, (-member * lines) % lanes, 1) if member else acc
            table = jnp.where(line == member, value, table)
        out[half] = turn(table)[:lines, :share]


def partner_routes(groups):
    if groups == 2 * GROUP_REACH:
        routes = []
        for step in (3, 1, 2):

            def target(source, step=step):
                team, member = divmod(source, 2)
                goal = team ^ step
                return goal * 2 + (member if team < goal else 1 - member)

            routes.append(([(source, target(source)) for source in range(groups)], True))
        routes.append(([(source, source ^ 1) for source in range(groups)], False))
        return routes
    return [
        ([(source, (source - hop) % groups) for source in range(groups)], False)
        for hop in range(1, GROUP_REACH + 1)
    ]


def body(inverse_cov, channel_keep_mask, partner_ids, band_starts):
    local_count, rows, channels = inverse_cov.shape
    width = channels // 2
    block = rows // 2
    bands = band_starts.shape[1]
    twice = 2 * bands
    groups, owners = lax.axis_size("bl"), lax.axis_size("bp")
    per_half = owners // 2
    assert local_count == 1 and width == 2 * rows and block == 128 == twice
    owner, group = lax.axis_index("bp"), lax.axis_index("bl")
    sc = jnp.stack([owner // per_half, owner % per_half, owner, group]).astype(jnp.int32)
    panel, diag, pack, info = pl.pallas_call(
        pack_kernel,
        in_specs=[SMEM, HBM, HBM, HBM, HBM],
        out_specs=[VMEM] * 4,
        out_shape=[
            jax.ShapeDtypeStruct((rows, width), f32),
            jax.ShapeDtypeStruct((rows, rows), f32),
            jax.ShapeDtypeStruct((4 * block + 8, block), f32),
            jax.ShapeDtypeStruct((8, block), f32),
        ],
        scratch_shapes=[
            pltpu.VMEM((rows, width), f32),
            pltpu.VMEM((1, channels), jnp.int32),
            pltpu.SMEM(partner_ids.shape, jnp.int32),
            pltpu.VMEM(band_starts.shape, jnp.int32),
            pltpu.SemaphoreType.DMA((4,)),
        ],
        compiler_params=params(16),
    )(sc, inverse_cov, channel_keep_mask, partner_ids, band_starts)

    other = lax.ppermute(diag, "bp", [(place, place ^ 1) for place in range(owners)])
    routes = partner_routes(groups)
    packs = [lax.ppermute(pack, "bl", route) for route, _ in routes]

    pairs = KINDS * (KINDS + 1) // 2
    shapes = [
        ((pairs * rows, rows), f32),
        ((KINDS * rows, KINDS * block), f32),
        ((twice, KINDS * rows), f32),
        ((twice, KINDS * block), f32),
        ((twice, KINDS * block), f32),
        ((twice, twice), f32),
        ((KINDS * rows, bands), bf16),
        ((KINDS * block, bands), bf16),
        ((KINDS * block, bands), bf16),
        ((bands, KINDS * rows), bf16),
        ((twice, width), bf16),
        ((twice, width), bf16),
    ]
    tables = pl.pallas_call(
        filter_kernel,
        in_specs=[SMEM, VMEM, VMEM, VMEM],
        out_specs=[VMEM] * len(shapes),
        out_shape=[jax.ShapeDtypeStruct(shape, kind) for shape, kind in shapes],
        scratch_shapes=[
            pltpu.VMEM((3 * width, width), bf16),
            pltpu.VMEM((3 * rows, KINDS * rows), bf16),
            pltpu.VMEM((3 * rows, KINDS * block), bf16),
            pltpu.VMEM((3 * rows, KINDS * block), bf16),
            pltpu.VMEM((KINDS * rows, 3 * rows), bf16),
        ],
        compiler_params=params(40),
        cost_estimate=pl.CostEstimate(
            flops=4_000_000_000, bytes_accessed=8 << 20, transcendentals=1 << 20
        ),
    )(sc, info, panel, other)

    scale = 1.0 / (4 * local_count * groups * WINDOW)
    share = bands // groups
    parts = pl.pallas_call(
        partial(contract_kernel, [both for _, both in routes], partner_ids.shape[1], scale, owners),
        in_specs=[VMEM] * (1 + len(routes) + len(shapes)),
        out_specs=VMEM,
        out_shape=jax.ShapeDtypeStruct((groups * owners, 1, block), f32),
        scratch_shapes=[
            pltpu.VMEM((KINDS * rows, bands), f32),
            pltpu.VMEM((twice, twice), f32),
        ],
        compiler_params=params(30),
    )(info, *packs, *tables)

    met = lax.all_to_all(parts, ("bl", "bp"), 0, 0, tiled=True)
    return pl.pallas_call(
        partial(gather_kernel, owners),
        in_specs=[VMEM],
        out_specs=VMEM,
        out_shape=jax.ShapeDtypeStruct((2, bands // owners, share), f32),
        compiler_params=params(8),
    )(met)


def solution(mesh):
    placed = (P("bl", "bp", None), P("bl", None), P("bl", None), P())
    return jax.shard_map(
        body, mesh=mesh, in_specs=placed, out_specs=P(None, "bp", "bl"), check_vma=False
    )
```

```python
from functools import partial

import jax
import jax.numpy as jnp
from jax import lax
from jax.experimental import pallas as pl
from jax.experimental.pallas import tpu as pltpu
from jax.sharding import PartitionSpec as P

WINDOW = 128
KINDS = 4
GROUP_REACH = 4

f32 = jnp.float32
bf16 = jnp.bfloat16
SMEM = pl.BlockSpec(memory_space=pltpu.SMEM)
VMEM = pl.BlockSpec(memory_space=pltpu.VMEM)
HBM = pl.BlockSpec(memory_space=pltpu.HBM)


def params(mib):
    return pltpu.CompilerParams(vmem_limit_bytes=mib << 20)


def dot(a, b):
    return jnp.dot(a, b, preferred_element_type=f32)


def split(x):
    high = x.astype(bf16)
    return high, (x - high.astype(f32)).astype(bf16)


def left3(x):
    high, low = split(x)
    return jnp.concatenate([high, low, high], axis=1)


def right3(x):
    high, low = split(x)
    return jnp.concatenate([high, high, low], axis=0)


def dot_t(a, b):
    return lax.dot_general(a, b, (((1,), (1,)), ((), ())), preferred_element_type=f32)


def iota(shape, dim):
    return lax.broadcasted_iota(jnp.int32, shape, dim)


def pack_kernel(
    sc, cov_hbm, keep_hbm, pid_hbm, starts_hbm, panel_out, diag_out, info_out, pack_out,
    cov, keep, pid, starts, sems,
):
    rows, width = cov.shape
    columns = pl.ds(pl.multiple_of(sc[0] * width, width), width)
    copies = [
        pltpu.make_async_copy(cov_hbm.at[0, :, columns], cov, sems.at[0]),
        pltpu.make_async_copy(keep_hbm, keep, sems.at[1]),
        pltpu.make_async_copy(pid_hbm, pid, sems.at[2]),
        pltpu.make_async_copy(starts_hbm, starts, sems.at[3]),
    ]
    for copy in copies:
        copy.start()
    for copy in copies:
        copy.wait()
    block = rows // 2
    first = sc[1] == 0
    marks = keep[...].astype(f32)
    half_marks = jnp.where(sc[0] == 0, marks[:, :width], marks[:, width:])
    row_marks = jnp.where(first, half_marks[:, :rows], half_marks[:, rows:])
    row_col = jnp.transpose(jnp.broadcast_to(row_marks, (128, rows)))[:, :1]
    masked = cov[...] * row_col * half_marks
    own = jnp.where(first, masked[:, :rows], masked[:, rows:])
    c0 = jnp.where(first, masked[:, 2 * block : 3 * block], masked[:, block : 2 * block])
    c1 = jnp.where(first, masked[:, 3 * block :], masked[:, :block])
    panel_out[:, :rows] = own
    panel_out[:, rows : rows + block] = c0
    panel_out[:, rows + block :] = c1
    d00, d01 = own[:block, :block], own[:block, block:]
    d10, d11 = own[block:, :block], own[block:, block:]
    diag_out[:block, :block] = jnp.where(first, d11, d00)
    diag_out[:block, block:] = jnp.where(first, d10, d01)
    diag_out[block:, :block] = jnp.where(first, d01, d10)
    diag_out[block:, block:] = jnp.where(first, d00, d11)
    above = iota((block, block), 0) < iota((block, block), 1)
    on = iota((block, block), 0) == iota((block, block), 1)
    line = iota((8, block), 0)
    info = jnp.where(line == 0, jnp.sum(jnp.where(on, d00, 0.0), axis=0, keepdims=True), 0.0)
    info = jnp.where(line == 1, sc[3].astype(f32), info)
    for slot in range(pid.shape[1]):
        info = jnp.where(line == 2 + slot, pid[0, slot].astype(f32), info)
    begin = jnp.where(sc[0] == 0, starts[0:1, :], starts[1:2, :]).astype(f32)
    info = jnp.where(line == 7, jnp.concatenate([begin, begin], axis=1), info)
    info_out[...] = info
    for at, value in enumerate((d01, jnp.where(above, d00, d11), c0[:block], c1[block:])):
        pack_out[at * block : (at + 1) * block] = value
    pack_out[4 * block :] = info


def turn(x):
    return jnp.transpose(x)


def decay(shape, dim):
    return -1.0 / (1 + iota(shape, dim) % KINDS).astype(f32)


def held(offset):
    return (offset >= 0) & (offset < WINDOW)


def edge_tools(sc, rows, block):
    first = sc[1] == 0

    def own_place(index):
        return index + jnp.where(first, 0, rows)

    def other_place(index):
        return jnp.where(first, index + rows, (index + block) % rows)

    def fade(place, shape, dim):
        return jnp.exp(jnp.abs(place.astype(f32) - (rows - 0.5)) * decay(shape, dim))

    return own_place, other_place, fade


def outside(offset, bands):
    shape = offset.shape
    reach = jnp.where(iota(shape, 0) >= bands, offset - WINDOW, -1.0 - offset)
    return jnp.where(
        reach >= 0, jnp.exp(jnp.where(reach >= 0, reach, 0.0) * decay(shape, 0)), 0.0
    )


def inside(offset, bands):
    shape = offset.shape
    reach = jnp.where(iota(shape, 0) >= bands, WINDOW - offset, offset + 1.0)
    return jnp.where(
        held(offset), jnp.exp(jnp.where(held(offset), reach, 0.0) * decay(shape, 0)), 0.0
    )


def prepare_kernel(
    sc, info, panel,
    td_out, to_out, hd_out, er_out, ec_out, eo_out, q_out, kc0, kc1,
    bd_out, b0_out, b1_out, br_out, rh_out, rl_out,
    p3, kr, kl,
):
    first = sc[1] == 0
    rows, width = panel.shape
    block = rows // 2
    twice = info.shape[1]
    bands = twice // 2
    own_place, other_place, fade = edge_tools(sc, rows, block)

    high, low = split(panel[...])
    for third, part in enumerate((high, high, low)):
        p3[third * rows : (third + 1) * rows, :] = part

    for chunk in range(2):
        shape = (block, rows)
        line = iota(shape, 0) + chunk * block
        lane = iota(shape, 1)
        spread = jnp.abs(line - lane).astype(f32)
        swapped = jnp.abs((line + block) % rows - (lane + block) % rows).astype(f32)
        cross = jnp.where(first, spread, swapped)
        here = chunk * block
        for kind in range(KINDS):
            at = slice(kind * rows, (kind + 1) * rows)
            high, low = split(jnp.exp(spread / -(1.0 + kind)))
            for third, part in enumerate((high, high, low)):
                kr[third * rows + here : third * rows + here + block, at] = part
            for third, part in enumerate((high, low, high)):
                kl[kind * rows + here : kind * rows + here + block,
                   third * rows : (third + 1) * rows] = part
            high, low = split(jnp.exp(cross / -(1.0 + kind)))
            at = slice(kind * block, (kind + 1) * block)
            for third, part in enumerate((high, high, low)):
                kc0[third * rows + here : third * rows + here + block, at] = part[:, :block]
                kc1[third * rows + here : third * rows + here + block, at] = part[:, block:]

    shape = (rows, twice)
    own_column = fade(own_place(iota(shape, 0)), shape, 1)
    other_column = fade(other_place(iota(shape, 0)), shape, 1)
    shape = (8, rows)
    own_row = fade(own_place(iota(shape, 1)), shape, 0)
    other_row = fade(other_place(iota(shape, 1)), shape, 0)

    begin = info[7:8, :]
    begin_column = turn(jnp.broadcast_to(begin, (twice, twice)))[:, :1]
    shape = (twice, rows)
    own_offset = own_place(iota(shape, 1)).astype(f32) - begin_column
    other_offset = other_place(iota(shape, 1)).astype(f32) - begin_column
    none = jnp.zeros((8, rows), f32)
    four = iota((8, rows), 0) < KINDS
    weights_own = jnp.concatenate(
        [outside(own_offset, bands), jnp.where(four, 0.0, own_row), none], axis=0
    )
    weights_other = jnp.concatenate(
        [outside(other_offset, bands), jnp.where(four, other_row, 0.0), none], axis=0
    )
    part = dot(left3(weights_own), p3[...])
    edge_c = part[:, rows:]
    edge_r = part[:, :rows] + dot(left3(weights_other), right3(turn(panel[:, rows:])))
    left_r = left3(edge_r)
    from_own = dot(left_r, right3(own_column))
    from_other = dot(left3(edge_c), right3(other_column))
    er_out[...] = from_own
    ec_out[...] = edge_c
    eo_out[...] = weights_other
    high, low = split(weights_own)
    q_out[...] = dot_t(left_r, jnp.concatenate([high, high, low], axis=1)[:twice])[:twice]
    for kind in range(KINDS):
        at = slice(kind * rows, (kind + 1) * rows)
        full = dot(left_r, kr[:, at])
        hd_out[:, at] = full
        near = full[twice : twice + 8]
        near = near + jnp.where(
            four, 0.0, from_other[twice : twice + 8, kind : kind + 1] * own_row[kind : kind + 1]
        )
        turned = turn(near)
        value = dot(kl[at, :], p3[...])
        carry = edge_r[twice + kind : twice + kind + 1, :]
        left_own = left3(value[:, :rows] + own_column[:, kind : kind + 1] * carry)
        left_other = left3(value[:, rows:])
        for second in range(kind, KINDS):
            here = slice(second * rows, (second + 1) * rows)
            spot = pair_index(kind, second) * rows
            td_out[spot : spot + rows, :] = (
                dot(left_own, kr[:, here])
                + turned[:, second : second + 1] * own_row[second : second + 1]
            )
        top = dot(left_other[:block], kc0[...])
        bottom = dot(left_other[block:], kc1[...])
        for second in range(KINDS):
            here = slice(second * block, (second + 1) * block)
            column = turned[:, KINDS + second : KINDS + second + 1]
            line = other_row[second : second + 1]
            to_out[kind * rows : kind * rows + block, here] = (
                top[:, here] + column[:block] * line[:, :block]
            )
            to_out[kind * rows + block : (kind + 1) * rows, here] = (
                bottom[:, here] + column[block:] * line[:, block:]
            )

    begins = begin[:, :bands]

    def boxes(count, place):
        shape = (KINDS * count, bands)
        index = iota(shape, 0)
        hit = held(place(index % count).astype(f32) - begins)
        hit = hit & (iota(shape, 1) % KINDS == index // count)
        return jnp.where(hit, 1.0, 0.0).astype(bf16)

    bd_out[...] = boxes(rows, own_place)
    b0_out[...] = boxes(block, other_place)
    b1_out[...] = boxes(block, lambda index: other_place(index + block))
    shape = (bands, KINDS * rows)
    index = iota(shape, 1)
    hit = held(own_place(index % rows).astype(f32) - begin_column[:bands])
    hit = hit & (iota(shape, 0) % KINDS == index // rows)
    br_out[...] = jnp.where(hit, 1.0, 0.0).astype(bf16)
    high, low = split(inside(own_offset, bands))
    rh_out[:, :rows] = high
    rl_out[:, :rows] = low
    high, low = split(inside(other_offset, bands))
    rh_out[:, rows:] = high
    rl_out[:, rows:] = low


def finish_kernel(
    sc, other, td, to, hd, er, ec, eo, q, kc0, kc1,
    td_out, to_out, hd_out, h0_out, h1_out, q_out,
):
    rows = other.shape[0]
    block = rows // 2
    twice = q.shape[0]
    own_place, other_place, fade = edge_tools(sc, rows, block)
    shape = (rows, twice)
    own_column = fade(own_place(iota(shape, 0)), shape, 1)
    other_column = fade(other_place(iota(shape, 0)), shape, 1)
    shape = (8, rows)
    own_row = fade(own_place(iota(shape, 1)), shape, 0)
    other_row = fade(other_place(iota(shape, 1)), shape, 0)
    edge_c = ec[...] + dot(left3(eo[...]), right3(other[...]))
    left_c = left3(edge_c)
    high, low = split(eo[...])
    q_out[...] = (
        q[...] + dot_t(left_c, jnp.concatenate([high, high, low], axis=1)[:twice])[:twice]
    )
    from_other = dot(left_c, right3(other_column))
    high0 = dot(left_c, kc0[...])
    high1 = dot(left_c, kc1[...])
    for kind in range(KINDS):
        at = slice(kind * rows, (kind + 1) * rows)
        hd_out[:, at] = (
            hd[:twice, at] + from_other[:twice, kind : kind + 1] * own_row[kind : kind + 1]
        )
        here = slice(kind * block, (kind + 1) * block)
        column = er[:twice, kind : kind + 1]
        line = other_row[kind : kind + 1]
        h0_out[:, here] = high0[:twice, here] + column * line[:, :block]
        h1_out[:, here] = high1[:twice, here] + column * line[:, block:]
        column = own_column[:, kind : kind + 1]
        for second in range(kind, KINDS):
            spot = pair_index(kind, second) * rows
            line = own_row[second : second + 1] * from_other[
                twice + second : twice + second + 1, kind : kind + 1
            ]
            td_out[spot : spot + rows, :] = td[spot : spot + rows, :] + column * line
        mid = kind * rows + block
        end = (kind + 1) * rows
        line = slice(twice + kind, twice + kind + 1)
        to_out[kind * rows : mid, :] = to[kind * rows : mid, :] + column[:block] * high0[line, :]
        to_out[mid:end, :] = to[mid:end, :] + column[block:] * high1[line, :]


def pair_index(kind, second):
    return kind * KINDS - kind * (kind - 1) // 2 + second - kind


def contract_kernel(peer_counts, slots, scale, owners, info, *refs):
    count = len(peer_counts)
    packs = refs[:count]
    td, to, hd, h0, h1, q, bd, b0, b1, br, rh, rl, out, m_box, final = refs[count:]
    rows = td.shape[1]
    block = rows // 2
    bands = bd.shape[1]
    twice = 2 * bands
    own = info[...]
    total = extra = 0.0
    for pack, both in zip(packs, peer_counts):
        aux = pack[4 * block :, :]
        weight = jnp.zeros_like(aux[:1])
        for slot in range(slots):
            at = slice(2 + slot, 3 + slot)
            weight = weight + jnp.where(aux[1:2] == own[at], 1.0, 0.0)
            if both:
                weight = weight + jnp.where(aux[at] == own[1:2], 1.0, 0.0)
        total = total + pack[: 4 * block, :] * weight
        extra = extra + aux[0:1, :] * weight
    upper = total[:block]
    tri = total[block : 2 * block]
    flipped = turn(tri)
    above = iota((block, block), 0) < iota((block, block), 1)
    on = iota((block, block), 0) == iota((block, block), 1)
    s00 = jnp.where(above, tri, jnp.where(on, extra, flipped))
    s11 = jnp.where(above, flipped, tri)
    s_own = jnp.concatenate(
        [
            jnp.concatenate([s00, upper], axis=1),
            jnp.concatenate([turn(upper), s11], axis=1),
        ],
        axis=0,
    )
    s_c0 = total[2 * block : 3 * block]
    s_c1 = total[3 * block :]
    half_own = 0.5 * s_own
    pair0 = jnp.concatenate([s_c0, s_c0], axis=1)
    pair1 = jnp.concatenate([s_c1, s_c1], axis=1)

    def boxed(x, box):
        high, low = split(x)
        return dot(high, box) + dot(low, box)

    for kind in range(KINDS):
        top, mid, end = kind * rows, kind * rows + block, (kind + 1) * rows
        acc = jnp.zeros((rows, bands), f32)
        acc_top = jnp.zeros((block, bands), f32)
        acc_low = jnp.zeros((block, bands), f32)
        for second in range(kind, KINDS):
            here = slice(second * rows, (second + 1) * rows)
            at = pair_index(kind, second) * rows
            value = half_own if second == kind else s_own
            acc = acc + boxed(value * td[at : at + rows, :], bd[here, :])
        for second in range(0, KINDS, 2):
            here = slice(second * block, (second + 2) * block)
            acc_top = acc_top + boxed(pair0 * to[top:mid, here], b0[here, :])
            acc_low = acc_low + boxed(pair1 * to[mid:end, here], b1[here, :])
        m_box[top:mid, :] = acc[:block] + acc_top
        m_box[mid:end, :] = acc[block:] + acc_low
    high, low = split(m_box[...])
    result = dot(br[...], high) + dot(br[...], low)

    reach = (rh[:, :rows], rl[:, :rows])
    reach0 = (rh[:, :block], rl[:, :block])
    reach1 = (rh[:, block:rows], rl[:, block:rows])
    over0 = (rh[:, rows : rows + block], rl[:, rows : rows + block])
    over1 = (rh[:, rows + block :], rl[:, rows + block :])

    def three(a, b, multiply):
        return multiply(a[0], b[0]) + multiply(a[0], b[1]) + multiply(a[1], b[0])

    part_own, part0, part1 = split(s_own), split(s_c0), split(s_c1)
    y_own = three(reach, part_own, dot)
    y_off = jnp.concatenate([three(over0, part0, dot_t), three(over1, part1, dot_t)], axis=1)
    y_0 = three(reach0, part0, dot)
    y_1 = three(reach1, part1, dot)
    fourth = three(split(0.5 * y_own + y_off), reach, dot_t) * q[...]
    y_own = y_own + y_off
    second = jnp.zeros((twice, bands), f32)
    for kind in range(KINDS):
        here = slice(kind * rows, (kind + 1) * rows)
        second = second + boxed(y_own * hd[:, here], bd[here, :])
        here = slice(kind * block, (kind + 1) * block)
        second = second + boxed(y_0 * h0[:, here], b0[here, :])
        second = second + boxed(y_1 * h1[:, here], b1[here, :])
    fourth = fourth[:bands] + fourth[bands:]
    result = result - second[:bands] - second[bands:] + fourth[:, :bands] + fourth[:, bands:]
    final[...] = jnp.zeros(final.shape, f32)
    final[:bands, :bands] = result
    whole = final[...]
    final[...] = (whole + turn(whole)) * scale

    groups = out.shape[0] // owners
    share, lines = bands // groups, bands // owners
    lane = iota((groups, final.shape[1]), 1)
    for owner in range(owners):
        row = jnp.zeros((groups, final.shape[1]), f32)
        for member in range(share):
            value = final[pl.ds(member, groups, stride=share), :]
            move = (member - owner) * lines % final.shape[1]
            value = pltpu.roll(value, move, 1) if move else value
            row = jnp.where(lane // lines == member, value, row)
        for group in range(groups):
            out[group * owners + owner] = row[group : group + 1]


def gather_kernel(owners, parts, out):
    per_half = owners // 2
    share, lines = out.shape[1], out.shape[2]
    lanes = parts.shape[2]
    for half in range(2):
        acc = None
        for first in range(0, parts.shape[0], owners):
            for place in range(per_half):
                value = parts[first + half * per_half + place]
                acc = value if acc is None else acc + value
        for member in range(share):
            value = pltpu.roll(acc, (-member * lines) % lanes, 1) if member else acc
            out[half, member : member + 1, :] = value[:, :lines]


def partner_routes(groups):
    if groups == 2 * GROUP_REACH:
        routes = []
        for step in (3, 1, 2):

            def target(source, step=step):
                team, member = divmod(source, 2)
                goal = team ^ step
                return goal * 2 + (member if team < goal else 1 - member)

            routes.append(([(source, target(source)) for source in range(groups)], True))
        routes.append(([(source, source ^ 1) for source in range(groups)], False))
        return routes
    return [
        ([(source, (source - hop) % groups) for source in range(groups)], False)
        for hop in range(1, GROUP_REACH + 1)
    ]


def in_hbm(value):
    return pltpu.with_memory_space_constraint(value, pltpu.HBM)


def body(inverse_cov, channel_keep_mask, partner_ids, band_starts):
    local_count, rows, channels = inverse_cov.shape
    width = channels // 2
    block = rows // 2
    bands = band_starts.shape[1]
    twice = 2 * bands
    groups, owners = lax.axis_size("bl"), lax.axis_size("bp")
    per_half = owners // 2
    assert local_count == 1 and width == 2 * rows and block == 128 == twice
    owner, group = lax.axis_index("bp"), lax.axis_index("bl")
    sc = jnp.stack([owner // per_half, owner % per_half, owner, group]).astype(jnp.int32)
    panel, diag, info, pack = pl.pallas_call(
        pack_kernel,
        in_specs=[SMEM, HBM, HBM, HBM, HBM],
        out_specs=[VMEM] * 4,
        out_shape=[
            jax.ShapeDtypeStruct((rows, width), f32),
            jax.ShapeDtypeStruct((rows, rows), f32),
            jax.ShapeDtypeStruct((8, block), f32),
            jax.ShapeDtypeStruct((4 * block + 8, block), f32),
        ],
        scratch_shapes=[
            pltpu.VMEM((rows, width), f32),
            pltpu.VMEM((1, channels), jnp.int32),
            pltpu.SMEM(partner_ids.shape, jnp.int32),
            pltpu.VMEM(band_starts.shape, jnp.int32),
            pltpu.SemaphoreType.DMA((4,)),
        ],
        compiler_params=params(16),
    )(
        sc,
        in_hbm(inverse_cov),
        in_hbm(channel_keep_mask),
        in_hbm(partner_ids),
        in_hbm(band_starts),
    )

    other = lax.ppermute(diag, "bp", [(place, place ^ 1) for place in range(owners)])
    routes = partner_routes(groups)
    arrived = [lax.ppermute(pack, "bl", route) for route, _ in routes]

    pairs = KINDS * (KINDS + 1) // 2
    lines = twice + 16
    shapes = [
        ((pairs * rows, rows), f32),
        ((KINDS * rows, KINDS * block), f32),
        ((lines, KINDS * rows), f32),
        ((lines, twice), f32),
        ((lines, rows), f32),
        ((lines, rows), f32),
        ((twice, twice), f32),
        ((3 * rows, KINDS * block), bf16),
        ((3 * rows, KINDS * block), bf16),
        ((KINDS * rows, bands), bf16),
        ((KINDS * block, bands), bf16),
        ((KINDS * block, bands), bf16),
        ((bands, KINDS * rows), bf16),
        ((twice, width), bf16),
        ((twice, width), bf16),
    ]
    begun = pl.pallas_call(
        prepare_kernel,
        in_specs=[SMEM, VMEM, VMEM],
        out_specs=[VMEM] * len(shapes),
        out_shape=[jax.ShapeDtypeStruct(shape, kind) for shape, kind in shapes],
        scratch_shapes=[
            pltpu.VMEM((3 * rows, width), bf16),
            pltpu.VMEM((3 * rows, KINDS * rows), bf16),
            pltpu.VMEM((KINDS * rows, 3 * rows), bf16),
        ],
        compiler_params=params(36),
        cost_estimate=pl.CostEstimate(
            flops=4_000_000_000, bytes_accessed=8 << 20, transcendentals=1 << 20
        ),
    )(sc, info, panel)
    ends = shapes[:2] + [
        ((twice, KINDS * rows), f32),
        ((twice, KINDS * block), f32),
        ((twice, KINDS * block), f32),
        ((twice, twice), f32),
    ]
    tables = pl.pallas_call(
        finish_kernel,
        in_specs=[SMEM] + [VMEM] * 10,
        out_specs=[VMEM] * len(ends),
        out_shape=[jax.ShapeDtypeStruct(shape, kind) for shape, kind in ends],
        input_output_aliases={2: 0, 3: 1},
        compiler_params=params(16),
        cost_estimate=pl.CostEstimate(
            flops=2_000_000_000, bytes_accessed=8 << 20, transcendentals=1 << 17
        ),
    )(sc, other, *begun[:9])
    tables = [*tables, *begun[9:]]

    scale = 1.0 / (4 * local_count * groups * WINDOW)
    share = bands // groups
    parts = pl.pallas_call(
        partial(
            contract_kernel, [both for _, both in routes], partner_ids.shape[1], scale, owners
        ),
        in_specs=[VMEM] * (1 + len(arrived) + len(tables)),
        out_specs=VMEM,
        out_shape=jax.ShapeDtypeStruct((groups * owners, 1, block), f32),
        scratch_shapes=[
            pltpu.VMEM((KINDS * rows, bands), f32),
            pltpu.VMEM((twice, twice), f32),
        ],
        compiler_params=params(30),
    )(info, *arrived, *tables)

    met = lax.all_to_all(parts, ("bl", "bp"), 0, 0, tiled=True)
    turned = pl.pallas_call(
        partial(gather_kernel, owners),
        in_specs=[VMEM],
        out_specs=VMEM,
        out_shape=jax.ShapeDtypeStruct((2, share, bands // owners), f32),
        compiler_params=params(8),
    )(met)
    return jnp.swapaxes(turned, 1, 2)


def solution(mesh):
    placed = (P("bl", "bp", None), P("bl", None), P("bl", None), P())
    return jax.shard_map(
        body, mesh=mesh, in_specs=placed, out_specs=P(None, "bp", "bl"), check_vma=False
    )
```

```python
from functools import partial

import jax
import jax.numpy as jnp
from jax import lax
from jax.experimental import pallas as pl
from jax.experimental.pallas import tpu as pltpu
from jax.sharding import PartitionSpec as P

WINDOW = 128
KINDS = 4
GROUP_REACH = 4

f32 = jnp.float32
bf16 = jnp.bfloat16
VMEM = pl.BlockSpec(memory_space=pltpu.VMEM)
HBM = pl.BlockSpec(memory_space=pltpu.HBM)


def position():
    owner, per_half = lax.axis_index("bp"), lax.axis_size("bp") // 2
    return owner // per_half, owner % per_half, lax.axis_index("bl")


def params(mib):
    return pltpu.CompilerParams(vmem_limit_bytes=mib << 20)


def dot(a, b):
    return jnp.dot(a, b, preferred_element_type=f32)


def split(x):
    high = x.astype(bf16)
    return high, (x - high.astype(f32)).astype(bf16)


def left3(x):
    high, low = split(x)
    return jnp.concatenate([high, low, high], axis=1)


def right3(x):
    high, low = split(x)
    return jnp.concatenate([high, high, low], axis=0)


def dot_t(a, b):
    return lax.dot_general(a, b, (((1,), (1,)), ((), ())), preferred_element_type=f32)


def iota(shape, dim):
    return lax.broadcasted_iota(jnp.int32, shape, dim)


def pack_kernel(
    cov_hbm, keep_hbm, pid_hbm, starts_hbm, panel_out, diag_out, info_out, pack_out,
    cov, keep, pid, starts, sems,
):
    rows, width = cov.shape
    half, place, group = position()
    columns = pl.ds(pl.multiple_of(half * width, width), width)
    copies = [
        pltpu.make_async_copy(cov_hbm.at[0, :, columns], cov, sems.at[0]),
        pltpu.make_async_copy(keep_hbm, keep, sems.at[1]),
        pltpu.make_async_copy(pid_hbm, pid, sems.at[2]),
        pltpu.make_async_copy(starts_hbm, starts, sems.at[3]),
    ]
    for copy in copies:
        copy.start()
    for copy in copies:
        copy.wait()
    block = rows // 2
    first = place == 0
    marks = keep[...].astype(f32)
    half_marks = jnp.where(half == 0, marks[:, :width], marks[:, width:])
    row_marks = jnp.where(first, half_marks[:, :rows], half_marks[:, rows:])
    row_col = jnp.transpose(jnp.broadcast_to(row_marks, (128, rows)))[:, :1]
    masked = cov[...] * row_col * half_marks
    own = jnp.where(first, masked[:, :rows], masked[:, rows:])
    c0 = jnp.where(first, masked[:, 2 * block : 3 * block], masked[:, block : 2 * block])
    c1 = jnp.where(first, masked[:, 3 * block :], masked[:, :block])
    panel_out[:, :rows] = own
    panel_out[:, rows : rows + block] = c0
    panel_out[:, rows + block :] = c1
    d00, d01 = own[:block, :block], own[:block, block:]
    d10, d11 = own[block:, :block], own[block:, block:]
    diag_out[:block, :block] = jnp.where(first, d11, d00)
    diag_out[:block, block:] = jnp.where(first, d10, d01)
    diag_out[block:, :block] = jnp.where(first, d01, d10)
    diag_out[block:, block:] = jnp.where(first, d00, d11)
    above = iota((block, block), 0) < iota((block, block), 1)
    on = iota((block, block), 0) == iota((block, block), 1)
    line = iota((8, block), 0)
    info = jnp.where(line == 0, jnp.sum(jnp.where(on, d00, 0.0), axis=0, keepdims=True), 0.0)
    info = jnp.where(line == 1, group.astype(f32), info)
    for slot in range(pid.shape[1]):
        info = jnp.where(line == 2 + slot, pid[:, slot : slot + 1].astype(f32), info)
    begin = jnp.where(half == 0, starts[0:1, :], starts[1:2, :]).astype(f32)
    info = jnp.where(line == 7, jnp.concatenate([begin, begin], axis=1), info)
    info_out[...] = info
    for at, value in enumerate((d01, jnp.where(above, d00, d11), c0[:block], c1[block:])):
        pack_out[at * block : (at + 1) * block] = value
    pack_out[4 * block :] = info


def turn(x):
    return jnp.transpose(x)


def decay(shape, dim):
    return -1.0 / (1 + iota(shape, dim) % KINDS).astype(f32)


def held(offset):
    return (offset >= 0) & (offset < WINDOW)


def edge_tools(first, rows, block):

    def own_place(index):
        return index + jnp.where(first, 0, rows)

    def other_place(index):
        return jnp.where(first, index + rows, (index + block) % rows)

    def fade(place, shape, dim):
        return jnp.exp(jnp.abs(place.astype(f32) - (rows - 0.5)) * decay(shape, dim))

    return own_place, other_place, fade


def outside(offset, bands):
    shape = offset.shape
    reach = jnp.where(iota(shape, 0) >= bands, offset - WINDOW, -1.0 - offset)
    return jnp.where(
        reach >= 0, jnp.exp(jnp.where(reach >= 0, reach, 0.0) * decay(shape, 0)), 0.0
    )


def inside(offset, bands):
    shape = offset.shape
    reach = jnp.where(iota(shape, 0) >= bands, WINDOW - offset, offset + 1.0)
    return jnp.where(
        held(offset), jnp.exp(jnp.where(held(offset), reach, 0.0) * decay(shape, 0)), 0.0
    )


def prepare_kernel(
    info, panel,
    td_out, to_out, hd_out, er_out, ec_out, eo_out, q_out, kc0, kc1,
    bx_out, br_out, bt_out, bl_out, rh_out, rl_out,
    p3, kr, kl,
):
    first = position()[1] == 0
    rows, width = panel.shape
    block = rows // 2
    twice = info.shape[1]
    bands = twice // 2
    own_place, other_place, fade = edge_tools(first, rows, block)

    high, low = split(panel[...])
    for third, part in enumerate((high, high, low)):
        p3[third * rows : (third + 1) * rows, :] = part

    for chunk in range(2):
        shape = (block, rows)
        line = iota(shape, 0) + chunk * block
        lane = iota(shape, 1)
        spread = jnp.abs(line - lane).astype(f32)
        swapped = jnp.abs((line + block) % rows - (lane + block) % rows).astype(f32)
        cross = jnp.where(first, spread, swapped)
        here = chunk * block
        for kind in range(KINDS):
            at = slice(kind * rows, (kind + 1) * rows)
            high, low = split(jnp.exp(spread / -(1.0 + kind)))
            for third, part in enumerate((high, high, low)):
                kr[third * rows + here : third * rows + here + block, at] = part
            for third, part in enumerate((high, low, high)):
                kl[kind * rows + here : kind * rows + here + block,
                   third * rows : (third + 1) * rows] = part
            high, low = split(jnp.exp(cross / -(1.0 + kind)))
            at = slice(kind * block, (kind + 1) * block)
            for third, part in enumerate((high, high, low)):
                kc0[third * rows + here : third * rows + here + block, at] = part[:, :block]
                kc1[third * rows + here : third * rows + here + block, at] = part[:, block:]

    shape = (rows, twice)
    own_column = fade(own_place(iota(shape, 0)), shape, 1)
    other_column = fade(other_place(iota(shape, 0)), shape, 1)
    shape = (8, rows)
    own_row = fade(own_place(iota(shape, 1)), shape, 0)
    other_row = fade(other_place(iota(shape, 1)), shape, 0)

    begin = info[7:8, :]
    begin_column = turn(jnp.broadcast_to(begin, (twice, twice)))[:, :1]
    shape = (twice, rows)
    own_offset = own_place(iota(shape, 1)).astype(f32) - begin_column
    other_offset = other_place(iota(shape, 1)).astype(f32) - begin_column
    none = jnp.zeros((8, rows), f32)
    four = iota((8, rows), 0) < KINDS
    weights_own = jnp.concatenate(
        [outside(own_offset, bands), jnp.where(four, 0.0, own_row), none], axis=0
    )
    weights_other = jnp.concatenate(
        [outside(other_offset, bands), jnp.where(four, other_row, 0.0), none], axis=0
    )
    part = dot(left3(weights_own), p3[...])
    edge_c = part[:, rows:]
    edge_r = part[:, :rows] + dot(left3(weights_other), right3(turn(panel[:, rows:])))
    left_r = left3(edge_r)
    from_own = dot(left_r, right3(own_column))
    from_other = dot(left3(edge_c), right3(other_column))
    er_out[...] = from_own
    ec_out[...] = edge_c
    eo_out[...] = weights_other
    high, low = split(weights_own)
    q_out[...] = dot_t(left_r, jnp.concatenate([high, high, low], axis=1)[:twice])[:twice]
    for kind in range(KINDS):
        at = slice(kind * rows, (kind + 1) * rows)
        full = dot(left_r, kr[:, at])
        hd_out[:, at] = full
        near = full[twice : twice + 8]
        near = near + jnp.where(
            four, 0.0, from_other[twice : twice + 8, kind : kind + 1] * own_row[kind : kind + 1]
        )
        turned = turn(near)
        value = dot(kl[at, :], p3[...])
        carry = edge_r[twice + kind : twice + kind + 1, :]
        left_own = left3(value[:, :rows] + own_column[:, kind : kind + 1] * carry)
        left_other = left3(value[:, rows:])
        for second in range(kind, KINDS):
            here = slice(second * rows, (second + 1) * rows)
            spot = pair_index(kind, second) * rows
            td_out[spot : spot + rows, :] = (
                dot(left_own, kr[:, here])
                + turned[:, second : second + 1] * own_row[second : second + 1]
            )
        top = dot(left_other[:block], kc0[...])
        bottom = dot(left_other[block:], kc1[...])
        for second in range(KINDS):
            here = slice(second * block, (second + 1) * block)
            column = turned[:, KINDS + second : KINDS + second + 1]
            line = other_row[second : second + 1]
            to_out[kind * rows : kind * rows + block, here] = (
                top[:, here] + column[:block] * line[:, :block]
            )
            to_out[kind * rows + block : (kind + 1) * rows, here] = (
                bottom[:, here] + column[block:] * line[:, block:]
            )

    begins = begin[:, :bands]

    def boxes(count, place):
        shape = (KINDS * count, bands)
        index = iota(shape, 0)
        hit = held(place(index % count).astype(f32) - begins)
        hit = hit & (iota(shape, 1) % KINDS == index // count)
        return jnp.where(hit, 1.0, 0.0).astype(bf16)

    def row_boxes(count, place):
        shape = (bands, 2 * KINDS * count)
        index = iota(shape, 1)
        hit = held(place(index % count).astype(f32) - begin_column[:bands])
        hit = hit & (iota(shape, 0) % KINDS == index // (2 * count))
        return jnp.where(hit, 1.0, 0.0).astype(bf16)

    cut = KINDS * rows
    bx_out[:cut, :] = boxes(rows, own_place)
    bx_out[cut : cut + KINDS * block, :] = boxes(block, other_place)
    bx_out[cut + KINDS * block :, :] = boxes(block, lambda index: other_place(index + block))
    br_out[...] = row_boxes(rows, own_place)
    bt_out[...] = row_boxes(block, own_place)
    bl_out[...] = row_boxes(block, lambda index: own_place(index + block))
    high, low = split(inside(own_offset, bands))
    rh_out[:, :rows] = high
    rl_out[:, :rows] = low
    high, low = split(inside(other_offset, bands))
    rh_out[:, rows:] = high
    rl_out[:, rows:] = low


def finish_kernel(
    other, td, to, hd, er, ec, eo, q, kc0, kc1,
    td_out, to_out, hd_out, h0_out, h1_out, q_out,
):
    rows = other.shape[0]
    block = rows // 2
    twice = q.shape[0]
    own_place, other_place, fade = edge_tools(position()[1] == 0, rows, block)
    shape = (rows, twice)
    own_column = fade(own_place(iota(shape, 0)), shape, 1)
    other_column = fade(other_place(iota(shape, 0)), shape, 1)
    shape = (8, rows)
    own_row = fade(own_place(iota(shape, 1)), shape, 0)
    other_row = fade(other_place(iota(shape, 1)), shape, 0)
    edge_c = ec[...] + dot(left3(eo[...]), right3(other[...]))
    left_c = left3(edge_c)
    high, low = split(eo[...])
    q_out[...] = (
        q[...] + dot_t(left_c, jnp.concatenate([high, high, low], axis=1)[:twice])[:twice]
    )
    from_other = dot(left_c, right3(other_column))
    high0 = dot(left_c, kc0[...])
    high1 = dot(left_c, kc1[...])
    for kind in range(KINDS):
        at = slice(kind * rows, (kind + 1) * rows)
        hd_out[:, at] = (
            hd[:twice, at] + from_other[:twice, kind : kind + 1] * own_row[kind : kind + 1]
        )
        here = slice(kind * block, (kind + 1) * block)
        column = er[:twice, kind : kind + 1]
        line = other_row[kind : kind + 1]
        h0_out[:, here] = high0[:twice, here] + column * line[:, :block]
        h1_out[:, here] = high1[:twice, here] + column * line[:, block:]
        column = own_column[:, kind : kind + 1]
        for second in range(kind, KINDS):
            spot = pair_index(kind, second) * rows
            line = own_row[second : second + 1] * from_other[
                twice + second : twice + second + 1, kind : kind + 1
            ]
            td_out[spot : spot + rows, :] = td[spot : spot + rows, :] + column * line
        mid = kind * rows + block
        end = (kind + 1) * rows
        line = slice(twice + kind, twice + kind + 1)
        to_out[kind * rows : mid, :] = to[kind * rows : mid, :] + column[:block] * high0[line, :]
        to_out[mid:end, :] = to[mid:end, :] + column[block:] * high1[line, :]


def pair_index(kind, second):
    return kind * KINDS - kind * (kind - 1) // 2 + second - kind


def contract_kernel(peer_counts, slots, scale, owners, info, *refs):
    count = len(peer_counts)
    packs = refs[:count]
    td, to, hd, h0, h1, q, bx, br, bt, bl, rh, rl, out, final = refs[count:]
    rows = td.shape[1]
    block = rows // 2
    bands = bx.shape[1]
    twice = 2 * bands
    own = info[...]
    total = extra = 0.0
    for pack, both in zip(packs, peer_counts):
        aux = pack[4 * block :, :]
        weight = jnp.zeros_like(aux[:1])
        for slot in range(slots):
            at = slice(2 + slot, 3 + slot)
            weight = weight + jnp.where(aux[1:2] == own[at], 1.0, 0.0)
            if both:
                weight = weight + jnp.where(aux[at] == own[1:2], 1.0, 0.0)
        total = total + pack[: 4 * block, :] * weight
        extra = extra + aux[0:1, :] * weight
    upper = total[:block]
    tri = total[block : 2 * block]
    flipped = turn(tri)
    above = iota((block, block), 0) < iota((block, block), 1)
    on = iota((block, block), 0) == iota((block, block), 1)
    s00 = jnp.where(above, tri, jnp.where(on, extra, flipped))
    s11 = jnp.where(above, flipped, tri)
    s_own = jnp.concatenate(
        [
            jnp.concatenate([s00, upper], axis=1),
            jnp.concatenate([turn(upper), s11], axis=1),
        ],
        axis=0,
    )
    s_c0 = total[2 * block : 3 * block]
    s_c1 = total[3 * block :]
    half_own = 0.5 * s_own
    pair0 = jnp.concatenate([s_c0, s_c0], axis=1)
    pair1 = jnp.concatenate([s_c1, s_c1], axis=1)

    def parts(values):
        return jnp.concatenate([part for value in values for part in split(value)], axis=0)

    pieces = range(0, KINDS * block, rows)
    sums = []
    for second in range(KINDS):
        products = []
        for kind in range(second + 1):
            at = pair_index(kind, second) * rows
            value = half_own if second == kind else s_own
            products.append(value * td[at : at + rows, :])
        sums.append(dot(br[:, : 2 * rows * (second + 1)], parts(products)))
    starts = range(0, KINDS * rows, rows)
    for at in pieces:
        products = [pair0 * to[top : top + block, at : at + rows] for top in starts]
        sums.append(dot(bt[...], parts(products)))
    for at in pieces:
        products = [pair1 * to[top + block : top + rows, at : at + rows] for top in starts]
        sums.append(dot(bl[...], parts(products)))

    def reach(at):
        return jnp.concatenate([rh[:, at], rl[:, at], rh[:, at]], axis=1)

    def thrice(x, axis):
        high, low = split(x)
        return jnp.concatenate([high, high, low], axis=axis)

    own_at = slice(0, rows)
    at0, at1 = slice(0, block), slice(block, rows)
    over0, over1 = slice(rows, rows + block), slice(rows + block, 2 * rows)
    y_own = dot(reach(own_at), thrice(s_own, 0))
    y_off = jnp.concatenate(
        [dot_t(reach(over0), thrice(s_c0, 1)), dot_t(reach(over1), thrice(s_c1, 1))], axis=1
    )
    y_0 = dot(reach(at0), thrice(s_c0, 0))
    y_1 = dot(reach(at1), thrice(s_c1, 0))
    fourth = dot_t(reach(own_at), thrice(0.5 * y_own + y_off, 1)) * q[...]
    y_own = y_own + y_off
    y_0 = jnp.concatenate([y_0, y_0], axis=1)
    y_1 = jnp.concatenate([y_1, y_1], axis=1)
    edges = [y_own * hd[:, at : at + rows] for at in starts]
    edges += [y_0 * h0[:, at : at + rows] for at in pieces]
    edges += [y_1 * h1[:, at : at + rows] for at in pieces]
    both = parts([jnp.concatenate(sums, axis=1), jnp.concatenate(edges, axis=1)])
    both = dot(both, bx[...])
    result = both[:bands] + both[bands:twice]
    second = both[twice : 2 * twice] + both[2 * twice :]
    fourth = fourth[:bands] + fourth[bands:]
    result = result - second[:bands] - second[bands:] + fourth[:, :bands] + fourth[:, bands:]
    final[...] = jnp.zeros(final.shape, f32)
    final[:bands, :bands] = result
    whole = final[...]
    final[...] = (whole + turn(whole)) * scale

    groups = out.shape[0] // owners
    share, lines = bands // groups, bands // owners
    lane = iota((groups, final.shape[1]), 1)
    for owner in range(owners):
        row = jnp.zeros((groups, final.shape[1]), f32)
        for member in range(share):
            value = final[pl.ds(member, groups, stride=share), :]
            move = (member - owner) * lines % final.shape[1]
            value = pltpu.roll(value, move, 1) if move else value
            row = jnp.where(lane // lines == member, value, row)
        for group in range(groups):
            out[group * owners + owner] = row[group : group + 1]


def gather_kernel(owners, parts, out):
    per_half = owners // 2
    share, lines = out.shape[1], out.shape[2]
    lanes = parts.shape[2]
    for half in range(2):
        acc = None
        for first in range(0, parts.shape[0], owners):
            for place in range(per_half):
                value = parts[first + half * per_half + place]
                acc = value if acc is None else acc + value
        for member in range(share):
            value = pltpu.roll(acc, (-member * lines) % lanes, 1) if member else acc
            out[half, member : member + 1, :] = value[:, :lines]


def partner_routes(groups):
    if groups == 2 * GROUP_REACH:
        routes = []
        for step in (3, 1, 2):

            def target(source, step=step):
                team, member = divmod(source, 2)
                goal = team ^ step
                return goal * 2 + (member if team < goal else 1 - member)

            routes.append(([(source, target(source)) for source in range(groups)], True))
        routes.append(([(source, source ^ 1) for source in range(groups)], False))
        return routes
    return [
        ([(source, (source - hop) % groups) for source in range(groups)], False)
        for hop in range(1, GROUP_REACH + 1)
    ]


def in_hbm(value):
    return pltpu.with_memory_space_constraint(value, pltpu.HBM)


def body(inverse_cov, channel_keep_mask, partner_ids, band_starts):
    local_count, rows, channels = inverse_cov.shape
    width = channels // 2
    block = rows // 2
    bands = band_starts.shape[1]
    twice = 2 * bands
    groups, owners = lax.axis_size("bl"), lax.axis_size("bp")
    assert local_count == 1 and width == 2 * rows and block == 128 == twice
    panel, diag, info, pack = pl.pallas_call(
        pack_kernel,
        in_specs=[HBM] * 4,
        out_specs=[VMEM] * 4,
        out_shape=[
            jax.ShapeDtypeStruct((rows, width), f32),
            jax.ShapeDtypeStruct((rows, rows), f32),
            jax.ShapeDtypeStruct((8, block), f32),
            jax.ShapeDtypeStruct((4 * block + 8, block), f32),
        ],
        scratch_shapes=[
            pltpu.VMEM((rows, width), f32),
            pltpu.VMEM((1, channels), jnp.int32),
            pltpu.VMEM(partner_ids.shape, jnp.int32),
            pltpu.VMEM(band_starts.shape, jnp.int32),
            pltpu.SemaphoreType.DMA((4,)),
        ],
        compiler_params=params(16),
    )(
        in_hbm(inverse_cov),
        in_hbm(channel_keep_mask),
        in_hbm(partner_ids),
        in_hbm(band_starts),
    )

    other = lax.ppermute(diag, "bp", [(place, place ^ 1) for place in range(owners)])
    routes = partner_routes(groups)
    arrived = [lax.ppermute(pack, "bl", route) for route, _ in routes]

    pairs = KINDS * (KINDS + 1) // 2
    lines = twice + 16
    shapes = [
        ((pairs * rows, rows), f32),
        ((KINDS * rows, KINDS * block), f32),
        ((lines, KINDS * rows), f32),
        ((lines, twice), f32),
        ((lines, rows), f32),
        ((lines, rows), f32),
        ((twice, twice), f32),
        ((3 * rows, KINDS * block), bf16),
        ((3 * rows, KINDS * block), bf16),
        ((2 * KINDS * rows, bands), bf16),
        ((bands, 2 * KINDS * rows), bf16),
        ((bands, 2 * KINDS * block), bf16),
        ((bands, 2 * KINDS * block), bf16),
        ((twice, width), bf16),
        ((twice, width), bf16),
    ]
    begun = pl.pallas_call(
        prepare_kernel,
        in_specs=[VMEM, VMEM],
        out_specs=[VMEM] * len(shapes),
        out_shape=[jax.ShapeDtypeStruct(shape, kind) for shape, kind in shapes],
        scratch_shapes=[
            pltpu.VMEM((3 * rows, width), bf16),
            pltpu.VMEM((3 * rows, KINDS * rows), bf16),
            pltpu.VMEM((KINDS * rows, 3 * rows), bf16),
        ],
        compiler_params=params(36),
        cost_estimate=pl.CostEstimate(
            flops=4_000_000_000, bytes_accessed=8 << 20, transcendentals=1 << 20
        ),
    )(info, panel)
    ends = shapes[:2] + [
        ((twice, KINDS * rows), f32),
        ((twice, KINDS * block), f32),
        ((twice, KINDS * block), f32),
        ((twice, twice), f32),
    ]
    tables = pl.pallas_call(
        finish_kernel,
        in_specs=[VMEM] * 10,
        out_specs=[VMEM] * len(ends),
        out_shape=[jax.ShapeDtypeStruct(shape, kind) for shape, kind in ends],
        input_output_aliases={1: 0, 2: 1},
        compiler_params=params(16),
        cost_estimate=pl.CostEstimate(
            flops=2_000_000_000, bytes_accessed=8 << 20, transcendentals=1 << 17
        ),
    )(other, *begun[:9])
    tables = [*tables, *begun[9:]]

    scale = 1.0 / (4 * local_count * groups * WINDOW)
    share = bands // groups
    parts = pl.pallas_call(
        partial(
            contract_kernel, [both for _, both in routes], partner_ids.shape[1], scale, owners
        ),
        in_specs=[VMEM] * (1 + len(arrived) + len(tables)),
        out_specs=VMEM,
        out_shape=jax.ShapeDtypeStruct((groups * owners, 1, block), f32),
        scratch_shapes=[pltpu.VMEM((twice, twice), f32)],
        compiler_params=params(30),
    )(info, *arrived, *tables)

    met = lax.all_to_all(parts, ("bl", "bp"), 0, 0, tiled=True)
    turned = pl.pallas_call(
        partial(gather_kernel, owners),
        in_specs=[VMEM],
        out_specs=VMEM,
        out_shape=jax.ShapeDtypeStruct((2, share, bands // owners), f32),
        compiler_params=params(8),
    )(met)
    return jnp.swapaxes(turned, 1, 2)


def solution(mesh):
    placed = (P("bl", "bp", None), P("bl", None), P("bl", None), P())
    return jax.shard_map(
        body, mesh=mesh, in_specs=placed, out_specs=P(None, "bp", "bl"), check_vma=False
    )
```

```python
from functools import partial

import jax
import jax.numpy as jnp
from jax import lax
from jax.experimental import pallas as pl
from jax.experimental.pallas import tpu as pltpu
from jax.sharding import PartitionSpec as P

WINDOW = 128
KINDS = 4
GROUP_REACH = 4

f32 = jnp.float32
bf16 = jnp.bfloat16
VMEM = pl.BlockSpec(memory_space=pltpu.VMEM)
HBM = pl.BlockSpec(memory_space=pltpu.HBM)


def position():
    owner, per_half = lax.axis_index("bp"), lax.axis_size("bp") // 2
    return owner // per_half, owner % per_half, lax.axis_index("bl")


def params(mib):
    return pltpu.CompilerParams(vmem_limit_bytes=mib << 20)


def dot(a, b):
    return jnp.dot(a, b, preferred_element_type=f32)


def split(x):
    high = x.astype(bf16)
    return high, (x - high.astype(f32)).astype(bf16)


def left3(x):
    high, low = split(x)
    return jnp.concatenate([high, low, high], axis=1)


def right3(x):
    high, low = split(x)
    return jnp.concatenate([high, high, low], axis=0)


def dot_t(a, b):
    return lax.dot_general(a, b, (((1,), (1,)), ((), ())), preferred_element_type=f32)


def iota(shape, dim):
    return lax.broadcasted_iota(jnp.int32, shape, dim)


def pack_kernel(
    cov_hbm, keep_hbm, pid_hbm, starts_hbm, panel_out, diag_out, info_out, pack_out,
    cov, keep, pid, starts, sems,
):
    rows, width = cov.shape
    half, place, group = position()
    columns = pl.ds(pl.multiple_of(half * width, width), width)
    copies = [
        pltpu.make_async_copy(cov_hbm.at[0, :, columns], cov, sems.at[0]),
        pltpu.make_async_copy(keep_hbm, keep, sems.at[1]),
        pltpu.make_async_copy(pid_hbm, pid, sems.at[2]),
        pltpu.make_async_copy(starts_hbm, starts, sems.at[3]),
    ]
    for copy in copies:
        copy.start()
    for copy in copies:
        copy.wait()
    block = rows // 2
    first = place == 0
    marks = keep[...].astype(f32)
    half_marks = jnp.where(half == 0, marks[:, :width], marks[:, width:])
    row_marks = jnp.where(first, half_marks[:, :rows], half_marks[:, rows:])
    row_col = jnp.transpose(jnp.broadcast_to(row_marks, (128, rows)))[:, :1]
    masked = cov[...] * row_col * half_marks
    own = jnp.where(first, masked[:, :rows], masked[:, rows:])
    c0 = jnp.where(first, masked[:, 2 * block : 3 * block], masked[:, block : 2 * block])
    c1 = jnp.where(first, masked[:, 3 * block :], masked[:, :block])
    panel_out[:, :rows] = own
    panel_out[:, rows : rows + block] = c0
    panel_out[:, rows + block :] = c1
    d00, d01 = own[:block, :block], own[:block, block:]
    d10, d11 = own[block:, :block], own[block:, block:]
    diag_out[:block, :block] = jnp.where(first, d11, d00)
    diag_out[:block, block:] = jnp.where(first, d10, d01)
    diag_out[block:, :block] = jnp.where(first, d01, d10)
    diag_out[block:, block:] = jnp.where(first, d00, d11)
    above = iota((block, block), 0) < iota((block, block), 1)
    on = iota((block, block), 0) == iota((block, block), 1)
    line = iota((8, block), 0)
    info = jnp.where(line == 0, jnp.sum(jnp.where(on, d00, 0.0), axis=0, keepdims=True), 0.0)
    info = jnp.where(line == 1, group.astype(f32), info)
    for slot in range(pid.shape[1]):
        info = jnp.where(line == 2 + slot, pid[:, slot : slot + 1].astype(f32), info)
    begin = jnp.where(half == 0, starts[0:1, :], starts[1:2, :]).astype(f32)
    info = jnp.where(line == 7, jnp.concatenate([begin, begin], axis=1), info)
    info_out[...] = info
    for at, value in enumerate((d01, jnp.where(above, d00, d11), c0[:block], c1[block:])):
        pack_out[at * block : (at + 1) * block] = value
    pack_out[4 * block :] = info


def turn(x):
    return jnp.transpose(x)


def decay(shape, dim):
    return -1.0 / (1 + iota(shape, dim) % KINDS).astype(f32)


def held(offset):
    return (offset >= 0) & (offset < WINDOW)


def edge_tools(first, rows, block):

    def own_place(index):
        return index + jnp.where(first, 0, rows)

    def other_place(index):
        return jnp.where(first, index + rows, (index + block) % rows)

    def fade(place, shape, dim):
        return jnp.exp(jnp.abs(place.astype(f32) - (rows - 0.5)) * decay(shape, dim))

    return own_place, other_place, fade


def outside(offset, bands):
    shape = offset.shape
    reach = jnp.where(iota(shape, 0) >= bands, offset - WINDOW, -1.0 - offset)
    return jnp.where(
        reach >= 0, jnp.exp(jnp.where(reach >= 0, reach, 0.0) * decay(shape, 0)), 0.0
    )


def inside(offset, bands):
    shape = offset.shape
    reach = jnp.where(iota(shape, 0) >= bands, WINDOW - offset, offset + 1.0)
    return jnp.where(
        held(offset), jnp.exp(jnp.where(held(offset), reach, 0.0) * decay(shape, 0)), 0.0
    )


def prepare_kernel(
    info, panel,
    td_out, to_out, hd_out, er_out, ec_out, eo_out, q_out, kc0, kc1,
    bx_out, br_out, bt_out, bl_out, rh_out, rl_out,
    p3, kr, kl,
):
    first = position()[1] == 0
    rows, width = panel.shape
    block = rows // 2
    twice = info.shape[1]
    bands = twice // 2
    own_place, other_place, fade = edge_tools(first, rows, block)

    high, low = split(panel[...])
    for third, part in enumerate((high, high, low)):
        p3[third * rows : (third + 1) * rows, :] = part

    for chunk in range(2):
        shape = (block, rows)
        line = iota(shape, 0) + chunk * block
        lane = iota(shape, 1)
        spread = jnp.abs(line - lane).astype(f32)
        swapped = jnp.abs((line + block) % rows - (lane + block) % rows).astype(f32)
        cross = jnp.where(first, spread, swapped)
        here = chunk * block
        for kind in range(KINDS):
            at = slice(kind * rows, (kind + 1) * rows)
            high, low = split(jnp.exp(spread / -(1.0 + kind)))
            for third, part in enumerate((high, high, low)):
                kr[third * rows + here : third * rows + here + block, at] = part
            for third, part in enumerate((high, low, high)):
                kl[kind * rows + here : kind * rows + here + block,
                   third * rows : (third + 1) * rows] = part
            high, low = split(jnp.exp(cross / -(1.0 + kind)))
            at = slice(kind * block, (kind + 1) * block)
            for third, part in enumerate((high, high, low)):
                kc0[third * rows + here : third * rows + here + block, at] = part[:, :block]
                kc1[third * rows + here : third * rows + here + block, at] = part[:, block:]

    shape = (rows, twice)
    own_column = fade(own_place(iota(shape, 0)), shape, 1)
    other_column = fade(other_place(iota(shape, 0)), shape, 1)
    shape = (8, rows)
    own_row = fade(own_place(iota(shape, 1)), shape, 0)
    other_row = fade(other_place(iota(shape, 1)), shape, 0)

    begin = info[7:8, :]
    begin_column = turn(jnp.broadcast_to(begin, (twice, twice)))[:, :1]
    shape = (twice, rows)
    own_offset = own_place(iota(shape, 1)).astype(f32) - begin_column
    other_offset = other_place(iota(shape, 1)).astype(f32) - begin_column
    none = jnp.zeros((8, rows), f32)
    four = iota((8, rows), 0) < KINDS
    weights_own = jnp.concatenate(
        [outside(own_offset, bands), jnp.where(four, 0.0, own_row), none], axis=0
    )
    weights_other = jnp.concatenate(
        [outside(other_offset, bands), jnp.where(four, other_row, 0.0), none], axis=0
    )
    part = dot(left3(weights_own), p3[...])
    edge_c = part[:, rows:]
    edge_r = part[:, :rows] + dot(left3(weights_other), right3(turn(panel[:, rows:])))
    left_r = left3(edge_r)
    from_own = dot(left_r, right3(own_column))
    from_other = dot(left3(edge_c), right3(other_column))
    er_out[...] = from_own
    ec_out[...] = edge_c
    eo_out[...] = weights_other
    high, low = split(weights_own)
    q_out[...] = dot_t(left_r, jnp.concatenate([high, high, low], axis=1)[:twice])[:twice]
    for kind in range(KINDS):
        at = slice(kind * rows, (kind + 1) * rows)
        full = dot(left_r, kr[:, at])
        hd_out[:, at] = full
        near = full[twice : twice + 8]
        near = near + jnp.where(
            four, 0.0, from_other[twice : twice + 8, kind : kind + 1] * own_row[kind : kind + 1]
        )
        turned = turn(near)
        value = dot(kl[at, :], p3[...])
        carry = edge_r[twice + kind : twice + kind + 1, :]
        left_own = left3(value[:, :rows] + own_column[:, kind : kind + 1] * carry)
        left_other = left3(value[:, rows:])
        for second in range(kind, KINDS):
            here = slice(second * rows, (second + 1) * rows)
            spot = pair_index(kind, second) * rows
            td_out[spot : spot + rows, :] = (
                dot(left_own, kr[:, here])
                + turned[:, second : second + 1] * own_row[second : second + 1]
            )
        top = dot(left_other[:block], kc0[...])
        bottom = dot(left_other[block:], kc1[...])
        for second in range(KINDS):
            here = slice(second * block, (second + 1) * block)
            column = turned[:, KINDS + second : KINDS + second + 1]
            line = other_row[second : second + 1]
            to_out[kind * rows : kind * rows + block, here] = (
                top[:, here] + column[:block] * line[:, :block]
            )
            to_out[kind * rows + block : (kind + 1) * rows, here] = (
                bottom[:, here] + column[block:] * line[:, block:]
            )

    begins = begin[:, :bands]

    def boxes(count, place):
        shape = (KINDS * count, bands)
        index = iota(shape, 0)
        hit = held(place(index % count).astype(f32) - begins)
        hit = hit & (iota(shape, 1) % KINDS == index // count)
        return jnp.where(hit, 1.0, 0.0).astype(bf16)

    def row_boxes(count, place):
        shape = (bands, 2 * KINDS * count)
        index = iota(shape, 1)
        hit = held(place(index % count).astype(f32) - begin_column[:bands])
        hit = hit & (iota(shape, 0) % KINDS == index // (2 * count))
        return jnp.where(hit, 1.0, 0.0).astype(bf16)

    cut = KINDS * rows
    bx_out[:cut, :] = boxes(rows, own_place)
    bx_out[cut : cut + KINDS * block, :] = boxes(block, other_place)
    bx_out[cut + KINDS * block :, :] = boxes(block, lambda index: other_place(index + block))
    br_out[...] = row_boxes(rows, own_place)
    bt_out[...] = row_boxes(block, own_place)
    bl_out[...] = row_boxes(block, lambda index: own_place(index + block))
    high, low = split(inside(own_offset, bands))
    rh_out[:, :rows] = high
    rl_out[:, :rows] = low
    high, low = split(inside(other_offset, bands))
    rh_out[:, rows:] = high
    rl_out[:, rows:] = low


def finish_kernel(
    other, td, to, hd, er, ec, eo, q, kc0, kc1,
    td_out, to_out, hd_out, h0_out, h1_out, q_out,
):
    rows = other.shape[0]
    block = rows // 2
    twice = q.shape[0]
    own_place, other_place, fade = edge_tools(position()[1] == 0, rows, block)
    shape = (rows, twice)
    own_column = fade(own_place(iota(shape, 0)), shape, 1)
    other_column = fade(other_place(iota(shape, 0)), shape, 1)
    shape = (8, rows)
    own_row = fade(own_place(iota(shape, 1)), shape, 0)
    other_row = fade(other_place(iota(shape, 1)), shape, 0)
    edge_c = ec[...] + dot(left3(eo[...]), right3(other[...]))
    left_c = left3(edge_c)
    high, low = split(eo[...])
    q_out[...] = (
        q[...] + dot_t(left_c, jnp.concatenate([high, high, low], axis=1)[:twice])[:twice]
    )
    from_other = dot(left_c, right3(other_column))
    high0 = dot(left_c, kc0[...])
    high1 = dot(left_c, kc1[...])
    for kind in range(KINDS):
        at = slice(kind * rows, (kind + 1) * rows)
        hd_out[:, at] = (
            hd[:twice, at] + from_other[:twice, kind : kind + 1] * own_row[kind : kind + 1]
        )
        here = slice(kind * block, (kind + 1) * block)
        column = er[:twice, kind : kind + 1]
        line = other_row[kind : kind + 1]
        h0_out[:, here] = high0[:twice, here] + column * line[:, :block]
        h1_out[:, here] = high1[:twice, here] + column * line[:, block:]
        column = own_column[:, kind : kind + 1]
        for second in range(kind, KINDS):
            spot = pair_index(kind, second) * rows
            line = own_row[second : second + 1] * from_other[
                twice + second : twice + second + 1, kind : kind + 1
            ]
            td_out[spot : spot + rows, :] = td[spot : spot + rows, :] + column * line
        mid = kind * rows + block
        end = (kind + 1) * rows
        line = slice(twice + kind, twice + kind + 1)
        to_out[kind * rows : mid, :] = to[kind * rows : mid, :] + column[:block] * high0[line, :]
        to_out[mid:end, :] = to[mid:end, :] + column[block:] * high1[line, :]


def pair_index(kind, second):
    return kind * KINDS - kind * (kind - 1) // 2 + second - kind


def contract_kernel(peer_counts, slots, scale, owners, info, *refs):
    count = len(peer_counts)
    packs = refs[:count]
    td, to, hd, h0, h1, q, bx, br, bt, bl, rh, rl, out, final = refs[count:]
    rows = td.shape[1]
    block = rows // 2
    bands = bx.shape[1]
    twice = 2 * bands
    own = info[...]
    total = extra = 0.0
    for pack, both in zip(packs, peer_counts):
        aux = pack[4 * block :, :]
        weight = jnp.zeros_like(aux[:1])
        for slot in range(slots):
            at = slice(2 + slot, 3 + slot)
            weight = weight + jnp.where(aux[1:2] == own[at], 1.0, 0.0)
            if both:
                weight = weight + jnp.where(aux[at] == own[1:2], 1.0, 0.0)
        total = total + pack[: 4 * block, :] * weight
        extra = extra + aux[0:1, :] * weight
    upper = total[:block]
    tri = total[block : 2 * block]
    flipped = turn(tri)
    above = iota((block, block), 0) < iota((block, block), 1)
    on = iota((block, block), 0) == iota((block, block), 1)
    s00 = jnp.where(above, tri, jnp.where(on, extra, flipped))
    s11 = jnp.where(above, flipped, tri)
    s_own = jnp.concatenate(
        [
            jnp.concatenate([s00, upper], axis=1),
            jnp.concatenate([turn(upper), s11], axis=1),
        ],
        axis=0,
    )
    s_c0 = total[2 * block : 3 * block]
    s_c1 = total[3 * block :]
    half_own = 0.5 * s_own
    pair0 = jnp.concatenate([s_c0, s_c0], axis=1)
    pair1 = jnp.concatenate([s_c1, s_c1], axis=1)

    def parts(values):
        return jnp.concatenate([part for value in values for part in split(value)], axis=0)

    pieces = range(0, KINDS * block, rows)
    sums = []
    for second in range(KINDS):
        products = []
        for kind in range(second + 1):
            at = pair_index(kind, second) * rows
            value = half_own if second == kind else s_own
            products.append(value * td[at : at + rows, :])
        sums.append(dot(br[:, : 2 * rows * (second + 1)], parts(products)))
    starts = range(0, KINDS * rows, rows)
    for at in pieces:
        products = [pair0 * to[top : top + block, at : at + rows] for top in starts]
        sums.append(dot(bt[...], parts(products)))
    for at in pieces:
        products = [pair1 * to[top + block : top + rows, at : at + rows] for top in starts]
        sums.append(dot(bl[...], parts(products)))

    def reach(at):
        return jnp.concatenate([rh[:, at], rl[:, at], rh[:, at]], axis=1)

    def thrice(x, axis):
        high, low = split(x)
        return jnp.concatenate([high, high, low], axis=axis)

    own_at = slice(0, rows)
    at0, at1 = slice(0, block), slice(block, rows)
    over0, over1 = slice(rows, rows + block), slice(rows + block, 2 * rows)
    y_own = dot(reach(own_at), thrice(s_own, 0))
    y_off = jnp.concatenate(
        [dot_t(reach(over0), thrice(s_c0, 1)), dot_t(reach(over1), thrice(s_c1, 1))], axis=1
    )
    y_0 = dot(reach(at0), thrice(s_c0, 0))
    y_1 = dot(reach(at1), thrice(s_c1, 0))
    fourth = dot_t(reach(own_at), thrice(0.5 * y_own + y_off, 1)) * q[...]
    y_own = y_own + y_off
    y_0 = jnp.concatenate([y_0, y_0], axis=1)
    y_1 = jnp.concatenate([y_1, y_1], axis=1)
    edges = [y_own * hd[:, at : at + rows] for at in starts]
    edges += [y_0 * h0[:, at : at + rows] for at in pieces]
    edges += [y_1 * h1[:, at : at + rows] for at in pieces]
    both = parts([jnp.concatenate(sums, axis=1), jnp.concatenate(edges, axis=1)])
    both = dot(both, bx[...])
    result = both[:bands] + both[bands:twice]
    second = both[twice : 2 * twice] + both[2 * twice :]
    fourth = fourth[:bands] + fourth[bands:]
    result = result - second[:bands] - second[bands:] + fourth[:, :bands] + fourth[:, bands:]
    final[...] = jnp.zeros(final.shape, f32)
    final[:bands, :bands] = result
    whole = final[...]
    final[...] = (whole + turn(whole)) * scale

    groups = out.shape[0] // owners
    share, lines = bands // groups, bands // owners
    lane = iota((groups, final.shape[1]), 1)
    for owner in range(owners):
        row = jnp.zeros((groups, final.shape[1]), f32)
        for member in range(share):
            value = final[pl.ds(member, groups, stride=share), :]
            move = (member - owner) * lines % final.shape[1]
            value = pltpu.roll(value, move, 1) if move else value
            row = jnp.where(lane // lines == member, value, row)
        for group in range(groups):
            out[group * owners + owner] = row[group : group + 1]


def gather_kernel(owners, parts, out):
    per_half = owners // 2
    share, lines = out.shape[1], out.shape[2]
    lanes = parts.shape[2]
    for half in range(2):
        acc = None
        for first in range(0, parts.shape[0], owners):
            for place in range(per_half):
                value = parts[first + half * per_half + place]
                acc = value if acc is None else acc + value
        for member in range(share):
            value = pltpu.roll(acc, (-member * lines) % lanes, 1) if member else acc
            out[half, member : member + 1, :] = value[:, :lines]


def partner_routes(groups):
    if groups == 2 * GROUP_REACH:
        routes = []
        for step in (3, 1, 2):

            def target(source, step=step):
                team, member = divmod(source, 2)
                goal = team ^ step
                return goal * 2 + (member if (team < goal) == (step == 3) else 1 - member)

            routes.append(([(source, target(source)) for source in range(groups)], True))
        routes.append(([(source, source ^ 1) for source in range(groups)], False))
        return routes
    return [
        ([(source, (source - hop) % groups) for source in range(groups)], False)
        for hop in range(1, GROUP_REACH + 1)
    ]


def in_hbm(value):
    return pltpu.with_memory_space_constraint(value, pltpu.HBM)


def body(inverse_cov, channel_keep_mask, partner_ids, band_starts):
    local_count, rows, channels = inverse_cov.shape
    width = channels // 2
    block = rows // 2
    bands = band_starts.shape[1]
    twice = 2 * bands
    groups, owners = lax.axis_size("bl"), lax.axis_size("bp")
    assert local_count == 1 and width == 2 * rows and block == 128 == twice
    panel, diag, info, pack = pl.pallas_call(
        pack_kernel,
        in_specs=[HBM] * 4,
        out_specs=[VMEM] * 4,
        out_shape=[
            jax.ShapeDtypeStruct((rows, width), f32),
            jax.ShapeDtypeStruct((rows, rows), f32),
            jax.ShapeDtypeStruct((8, block), f32),
            jax.ShapeDtypeStruct((4 * block + 8, block), f32),
        ],
        scratch_shapes=[
            pltpu.VMEM((rows, width), f32),
            pltpu.VMEM((1, channels), jnp.int32),
            pltpu.VMEM(partner_ids.shape, jnp.int32),
            pltpu.VMEM(band_starts.shape, jnp.int32),
            pltpu.SemaphoreType.DMA((4,)),
        ],
        compiler_params=params(16),
    )(
        in_hbm(inverse_cov),
        in_hbm(channel_keep_mask),
        in_hbm(partner_ids),
        in_hbm(band_starts),
    )

    other = lax.ppermute(diag, "bp", [(place, place ^ 1) for place in range(owners)])
    routes = partner_routes(groups)
    arrived = [lax.ppermute(pack, "bl", route) for route, _ in routes]

    pairs = KINDS * (KINDS + 1) // 2
    lines = twice + 16
    shapes = [
        ((pairs * rows, rows), f32),
        ((KINDS * rows, KINDS * block), f32),
        ((lines, KINDS * rows), f32),
        ((lines, twice), f32),
        ((lines, rows), f32),
        ((lines, rows), f32),
        ((twice, twice), f32),
        ((3 * rows, KINDS * block), bf16),
        ((3 * rows, KINDS * block), bf16),
        ((2 * KINDS * rows, bands), bf16),
        ((bands, 2 * KINDS * rows), bf16),
        ((bands, 2 * KINDS * block), bf16),
        ((bands, 2 * KINDS * block), bf16),
        ((twice, width), bf16),
        ((twice, width), bf16),
    ]
    begun = pl.pallas_call(
        prepare_kernel,
        in_specs=[VMEM, VMEM],
        out_specs=[VMEM] * len(shapes),
        out_shape=[jax.ShapeDtypeStruct(shape, kind) for shape, kind in shapes],
        scratch_shapes=[
            pltpu.VMEM((3 * rows, width), bf16),
            pltpu.VMEM((3 * rows, KINDS * rows), bf16),
            pltpu.VMEM((KINDS * rows, 3 * rows), bf16),
        ],
        compiler_params=params(36),
        cost_estimate=pl.CostEstimate(
            flops=4_000_000_000, bytes_accessed=8 << 20, transcendentals=1 << 20
        ),
    )(info, panel)
    ends = shapes[:2] + [
        ((twice, KINDS * rows), f32),
        ((twice, KINDS * block), f32),
        ((twice, KINDS * block), f32),
        ((twice, twice), f32),
    ]
    tables = pl.pallas_call(
        finish_kernel,
        in_specs=[VMEM] * 10,
        out_specs=[VMEM] * len(ends),
        out_shape=[jax.ShapeDtypeStruct(shape, kind) for shape, kind in ends],
        input_output_aliases={1: 0, 2: 1},
        compiler_params=params(16),
        cost_estimate=pl.CostEstimate(
            flops=2_000_000_000, bytes_accessed=8 << 20, transcendentals=1 << 17
        ),
    )(other, *begun[:9])
    tables = [*tables, *begun[9:]]

    scale = 1.0 / (4 * local_count * groups * WINDOW)
    share = bands // groups
    parts = pl.pallas_call(
        partial(
            contract_kernel, [both for _, both in routes], partner_ids.shape[1], scale, owners
        ),
        in_specs=[VMEM] * (1 + len(arrived) + len(tables)),
        out_specs=VMEM,
        out_shape=jax.ShapeDtypeStruct((groups * owners, 1, block), f32),
        scratch_shapes=[pltpu.VMEM((twice, twice), f32)],
        compiler_params=params(30),
    )(info, *arrived, *tables)

    met = lax.all_to_all(parts, ("bl", "bp"), 0, 0, tiled=True)
    turned = pl.pallas_call(
        partial(gather_kernel, owners),
        in_specs=[VMEM],
        out_specs=VMEM,
        out_shape=jax.ShapeDtypeStruct((2, share, bands // owners), f32),
        compiler_params=params(8),
    )(met)
    return jnp.swapaxes(turned, 1, 2)


def solution(mesh):
    placed = (P("bl", "bp", None), P("bl", None), P("bl", None), P())
    return jax.shard_map(
        body, mesh=mesh, in_specs=placed, out_specs=P(None, "bp", "bl"), check_vma=False
    )
```
